64 devices in a mesh: data: 4 (over x, y), stage: 16 (over z, core).
Axes of the slice: x: 2, y: 2, z: 8, core: 2. Of those that a mesh axis runs over, the one named last changes fastest.
The devices are a block of a 4x4x8 slice.
Arguments:
- x_rows: bfloat16 [16384, 576], P(('data', 'stage')), parts along dimension 0
- w_head: bfloat16 [49152, 576], P('stage')
- labels: int32 [16384], P('data'), parts along dimension 0
- loss_mask: int32 [16384], P('data'), parts along dimension 0
- w_embed: bfloat16 [49152, 576], P('stage')
- next_ids: int32 [16384], P('data'), parts along dimension 0
- stage_acts: bfloat16 [64, 4096, 576], P(('data', 'stage')), parts along dimension 0
- mlp_in: bfloat16 [16, 2, 576, 1536], P('stage')
- mlp_out: bfloat16 [16, 2, 1536, 576], P('stage')
Outputs:
- output 1: float32 [4], P('data'), parts along dimension 0
- output 2: float32 [16384, 576], P(('data', 'stage')), parts along dimension 0
- output 3: bfloat16 [196608, 576], P(('data', 'stage')), parts along dimension 0
- output 4: bfloat16 [16384, 576], P(('data', 'stage')), parts along dimension 0
- output 5: bfloat16 [64, 4096, 576], P(('data', 'stage')), parts along dimension 0
There are 4 independent parts. The reference program is written for one: setup_inputs(seed, part) draws one part's arguments, and reference() takes and returns one part's arrays. A program takes and returns all parts, laid end to end along the dimension named above; an argument that names none is the same for every part.
All inputs are finite; a program needn't handle non-finite values.
Results may differ from the reference program's by a relative error of at most 0.00125.
Values are sent between devices in bfloat16 or wider.
A program may use at most 768 MiB of HBM per device.

```python
import jax
import jax.numpy as jnp
from jax import lax

TOKENS = 4096
MODEL_DIM = 576
VOCAB_SIZE = 49152
HIDDEN_DIM = 1536
NUM_STAGES = 16
SHARD_ROWS = VOCAB_SIZE // NUM_STAGES


def setup_inputs(seed: int = 0, part: int = 0) -> dict:
    shared = jax.random.split(jax.random.key(seed + 1), 4)
    part_keys = jax.random.split(jax.random.fold_in(jax.random.key(seed), part), 5)
    x_rows = jax.random.normal(part_keys[0], (TOKENS, MODEL_DIM), jnp.float32)
    w_head = jax.random.normal(shared[0], (VOCAB_SIZE, MODEL_DIM), jnp.float32) * (3.0 * MODEL_DIM ** -0.5)
    labels = jax.random.randint(part_keys[1], (TOKENS,), 0, VOCAB_SIZE, dtype=jnp.int32)
    loss_mask = (jax.random.randint(part_keys[2], (TOKENS,), 0, 10, dtype=jnp.int32) > 0).astype(jnp.int32)
    w_embed = jax.random.normal(shared[1], (VOCAB_SIZE, MODEL_DIM), jnp.float32)
    next_ids = jax.random.randint(part_keys[3], (TOKENS,), 0, VOCAB_SIZE, dtype=jnp.int32)
    stage_acts = jax.random.normal(part_keys[4], (NUM_STAGES, TOKENS, MODEL_DIM), jnp.float32)
    mlp_in = jax.random.normal(shared[2], (NUM_STAGES, 2, MODEL_DIM, HIDDEN_DIM), jnp.float32) * MODEL_DIM ** -0.5
    mlp_out = jax.random.normal(shared[3], (NUM_STAGES, 2, HIDDEN_DIM, MODEL_DIM), jnp.float32) * HIDDEN_DIM ** -0.5
    return {
        'x_rows': x_rows.astype(jnp.bfloat16),
        'w_head': w_head.astype(jnp.bfloat16),
        'labels': labels,
        'loss_mask': loss_mask,
        'w_embed': w_embed.astype(jnp.bfloat16),
        'next_ids': next_ids,
        'stage_acts': stage_acts.astype(jnp.bfloat16),
        'mlp_in': mlp_in.astype(jnp.bfloat16),
        'mlp_out': mlp_out.astype(jnp.bfloat16),
    }


def reference(x_rows, w_head, labels, loss_mask, w_embed, next_ids, stage_acts, mlp_in, mlp_out):
    head_shards = w_head.reshape(NUM_STAGES, SHARD_ROWS, MODEL_DIM)
    offsets = jnp.arange(NUM_STAGES, dtype=jnp.int32) * SHARD_ROWS
    col_ids = jnp.arange(SHARD_ROWS, dtype=jnp.int32)

    def shard_logits(w_shard, offset):
        logits = jnp.dot(x_rows, w_shard.T, preferred_element_type=jnp.float32)
        label_hit = col_ids[None, :] == (labels - offset)[:, None]
        return logits, label_hit

    def shard_stats(pair):
        logits, label_hit = shard_logits(pair[0], pair[1])
        local_max = jnp.max(logits, axis=1)
        local_sum = jnp.sum(jnp.exp(logits - local_max[:, None]), axis=1)
        target = jnp.sum(jnp.where(label_hit, logits, 0.0), axis=1)
        return local_max, local_sum, target

    shard_max, shard_sum, shard_target = lax.map(shard_stats, (head_shards, offsets))
    row_max = jnp.max(shard_max, axis=0)
    partition = jnp.sum(shard_sum * jnp.exp(shard_max - row_max[None, :]), axis=0)
    target_logit = jnp.sum(shard_target, axis=0)
    weight = loss_mask.astype(jnp.float32)
    token_count = jnp.maximum(jnp.sum(weight), 1.0)
    loss_value = jnp.sum(weight * (jnp.log(partition) + row_max - target_logit)) / token_count
    row_scale = weight / token_count

    def shard_grads(grad_acc, pair):
        logits, label_hit = shard_logits(pair[0], pair[1])
        soft_probs = jnp.exp(logits - row_max[:, None]) / partition[:, None]
        grad_logits = ((soft_probs - label_hit.astype(jnp.float32)) * row_scale[:, None]).astype(jnp.bfloat16)
        grad_acc = grad_acc + jnp.dot(grad_logits, pair[0], preferred_element_type=jnp.float32)
        grad_shard = jnp.dot(grad_logits.T, x_rows, preferred_element_type=jnp.float32).astype(jnp.bfloat16)
        return grad_acc, grad_shard

    grad_x, grad_head = lax.scan(shard_grads, jnp.zeros((TOKENS, MODEL_DIM), jnp.float32), (head_shards, offsets))
    grad_head = grad_head.reshape(VOCAB_SIZE, MODEL_DIM)
    embed_rows = jnp.take(w_embed, next_ids, axis=0)

    def mlp_stage(triple):
        hidden, up_pair, down_pair = triple
        for layer_idx in range(2):
            pre_act = jnp.dot(hidden, up_pair[layer_idx], preferred_element_type=jnp.float32)
            gelu_out = jax.nn.gelu(pre_act, approximate=True).astype(jnp.bfloat16)
            hidden = (hidden.astype(jnp.float32) + jnp.dot(gelu_out, down_pair[layer_idx], preferred_element_type=jnp.float32)).astype(jnp.bfloat16)
        return hidden

    middle = lax.map(mlp_stage, (stage_acts[1:NUM_STAGES - 1], mlp_in[1:NUM_STAGES - 1], mlp_out[1:NUM_STAGES - 1]))
    stage_out = jnp.concatenate([stage_acts[:1], middle, stage_acts[NUM_STAGES - 1:]], axis=0)
    return loss_value.reshape(1), grad_x, grad_head, embed_rows, stage_out
```

```python
import functools

import jax
import jax.numpy as jnp
from jax import lax
from jax.experimental import pallas as pl
from jax.experimental.pallas import tpu as pltpu
from jax.sharding import PartitionSpec as P

F32 = jnp.float32
BF16 = jnp.bfloat16
MESH = pl.DeviceIdType.MESH
CHUNK = 512
GROUP = 2
MIB = 1024 * 1024


def mm(a, b, ca, cb):
    return lax.dot_general(a, b, (((ca,), (cb,)), ((), ())), preferred_element_type=F32)


def params(limit, **kw):
    return pltpu.CompilerParams(vmem_limit_bytes=limit * MIB, **kw)


def cost(flops, nbytes):
    return pl.CostEstimate(flops=int(flops), bytes_accessed=int(nbytes), transcendentals=0)


def transpose_into(dst_ref, src, step):
    for c in range(0, src.shape[1], step):
        dst_ref[pl.ds(c, step), :] = src[:, c:c + step].T


def side_by_side(ref):
    return jnp.concatenate([ref[b] for b in range(ref.shape[0])], axis=1)


def gelu(x):
    k = 0.7978845608028654
    inner = x * (k + (k * 0.044715) * (x * x))
    half = 0.5 * x
    return half + half * jnp.tanh(inner)


def mlp_kernel(a_ref, up_ref, down_ref, y_ref, upt_ref):
    layers = up_ref.shape[0]
    stage = lax.axis_index('stage')
    middle = (stage > 0) & (stage < lax.axis_size('stage') - 1)

    @pl.when(pl.program_id(0) == 0)
    def _():
        for i in range(layers):
            transpose_into(upt_ref.at[i], up_ref[i], 256)

    @pl.when(middle)
    def _():
        h = a_ref[...]
        for i in range(layers):
            u = jnp.concatenate(
                [gelu(mm(upt_ref[i, pl.ds(c, 512), :], h, 1, 0)).astype(BF16) for c in range(0, up_ref.shape[2], 512)], axis=0)
            h = (h.astype(F32) + mm(down_ref[i], u, 1, 0)).astype(BF16)
        y_ref[...] = h

    @pl.when(jnp.logical_not(middle))
    def _():
        y_ref[...] = a_ref[...]


def mlp(at, up, down):
    dim, tokens = at.shape
    layers, _, hidden = up.shape
    tile = 512
    return pl.pallas_call(
        mlp_kernel,
        grid=(tokens // tile,),
        in_specs=[
            pl.BlockSpec((dim, tile), lambda i: (0, i)),
            pl.BlockSpec((layers, dim, hidden), lambda i: (0, 0, 0)),
            pl.BlockSpec((layers, dim, hidden), lambda i: (0, 0, 0)),
        ],
        out_specs=pl.BlockSpec((dim, tile), lambda i: (0, i)),
        out_shape=jax.ShapeDtypeStruct((dim, tokens), BF16),
        scratch_shapes=[pltpu.VMEM((layers, hidden, dim), BF16)],
        compiler_params=params(48),
        cost_estimate=cost(4 * layers * tokens * dim * hidden, 4 * tokens * dim + 4 * layers * dim * hidden),
        name='mlp',
    )(at, up, down)


def embed_kernel(ids_ref, et_ref, out_ref):
    rows = et_ref.shape[1]
    tok = ids_ref.shape[2]
    index = lax.broadcasted_iota(jnp.int32, (rows, GROUP * tok), 0)
    hot = jnp.where(index == side_by_side(ids_ref), 1.0, 0.0).astype(BF16)
    out = mm(et_ref[...], hot, 1, 0).astype(BF16)
    for b in range(GROUP):
        out_ref[b] = out[:, b * tok:(b + 1) * tok]


def embed(ids, et):
    n, _, tok = ids.shape
    dim, rows = et.shape
    return pl.pallas_call(
        embed_kernel,
        grid=(n // GROUP,),
        in_specs=[
            pl.BlockSpec((GROUP, 1, tok), lambda i: (i, 0, 0)),
            pl.BlockSpec((dim, rows), lambda i: (0, 0)),
        ],
        out_specs=pl.BlockSpec((GROUP, dim, tok), lambda i: (i, 0, 0)),
        out_shape=jax.ShapeDtypeStruct((n, dim, tok), BF16),
        compiler_params=params(48),
        cost_estimate=cost(2 * n * tok * dim * rows, 2 * dim * (n * tok + rows)),
        name='embed',
    )(ids, et)


def logits_kernel(wt_ref, x_ref, lab_ref, e_ref, cm_ref, st_ref, w_ref):
    rows = wt_ref.shape[1]
    tok = x_ref.shape[2]

    @pl.when(pl.program_id(0) == 0)
    def _():
        transpose_into(w_ref, wt_ref, 256)

    x = side_by_side(x_ref)
    lab = side_by_side(lab_ref)
    index = lax.broadcasted_iota(jnp.int32, (CHUNK, GROUP * tok), 0)
    maxes, sums = [], []
    target = jnp.zeros((1, GROUP * tok), F32)
    for c in range(rows // CHUNK):
        sl = pl.ds(c * CHUNK, CHUNK)
        z = mm(w_ref[sl, :], x, 1, 0)
        m = jnp.max(z, axis=0, keepdims=True)
        e = jnp.exp(z - m)
        for b in range(GROUP):
            e_ref[b, sl, :] = e[:, b * tok:(b + 1) * tok]
        maxes.append(m)
        sums.append(jnp.sum(e, axis=0, keepdims=True))
        target += jnp.sum(jnp.where(index == lab - c * CHUNK, z, 0.0), axis=0, keepdims=True)
    m = functools.reduce(jnp.maximum, maxes)
    s = sum(si * jnp.exp(mi - m) for mi, si in zip(maxes, sums))
    cm = jnp.concatenate(maxes + [jnp.zeros((8 - len(maxes), GROUP * tok), F32)], axis=0)
    st = jnp.concatenate([m, s, target, jnp.zeros((5, GROUP * tok), F32)], axis=0)
    for b in range(GROUP):
        cm_ref[b] = cm[:, b * tok:(b + 1) * tok]
        st_ref[b] = st[:, b * tok:(b + 1) * tok]


def logits(wt, x, lab):
    dim, rows = wt.shape
    n, _, tok = x.shape
    block = lambda r, c: pl.BlockSpec((GROUP, r, c), lambda i: (i, 0, 0))
    return pl.pallas_call(
        logits_kernel,
        grid=(n // GROUP,),
        in_specs=[pl.BlockSpec((dim, rows), lambda i: (0, 0)), block(dim, tok), block(1, tok)],
        out_specs=[block(rows, tok), block(8, tok), block(8, tok)],
        out_shape=[
            jax.ShapeDtypeStruct((n, rows, tok), F32),
            jax.ShapeDtypeStruct((n, 8, tok), F32),
            jax.ShapeDtypeStruct((n, 8, tok), F32),
        ],
        scratch_shapes=[pltpu.VMEM((rows, dim), BF16)],
        compiler_params=params(56),
        cost_estimate=cost(2 * n * tok * dim * rows, 4 * n * tok * rows),
        name='logits',
    )(wt, x, lab)


def stats_kernel(n, st_ref, mask_ref, out_ref, loss_ref, got, every, send1, recv1, send2, recv2):
    me = lax.axis_index('stage')
    barrier = pltpu.get_barrier_semaphore()
    peers = [lax.rem(me + d, n) for d in range(n)]
    for d in range(1, n):
        pl.semaphore_signal(barrier, inc=1, device_id={'stage': peers[d]}, device_id_type=MESH)
    pl.semaphore_wait(barrier, n - 1)

    first = []
    for d in range(1, n):
        first.append(pltpu.make_async_remote_copy(
            src_ref=st_ref.at[peers[d]], dst_ref=got.at[d], send_sem=send1.at[d], recv_sem=recv1.at[d],
            device_id={'stage': peers[d]}, device_id_type=MESH))
        first[-1].start()
    weight = mask_ref[...]
    count = jnp.maximum(jnp.sum(weight, keepdims=True)[0], 1.0)
    for copy in first:
        copy.wait()
    parts = [st_ref[me]] + [got[d] for d in range(1, n)]
    m = functools.reduce(jnp.maximum, [p[0:1] for p in parts])
    total = sum(p[1:2] * jnp.exp(p[0:1] - m) for p in parts)
    target = sum(p[2:3] for p in parts)
    w = mask_ref[me]
    scale = w / count
    term = w * (jnp.log(total) + m - target)
    mine = jnp.concatenate([m, scale / total, scale, term, jnp.zeros((4, m.shape[1]), F32)], axis=0)
    every[me] = mine
    second = []
    for d in range(1, n):
        second.append(pltpu.make_async_remote_copy(
            src_ref=every.at[me], dst_ref=every.at[me], send_sem=send2.at[d], recv_sem=recv2.at[d],
            device_id={'stage': peers[d]}, device_id_type=MESH))
        second[-1].start()
    for copy in second:
        copy.wait()
    out_ref[...] = every[...]
    loss_ref[...] = jnp.broadcast_to(jnp.sum(every[:, 3, :], keepdims=True) / count, loss_ref.shape)


def stats(st, mask):
    n, _, tok = st.shape
    vmem = pl.BlockSpec(memory_space=pltpu.VMEM)
    return pl.pallas_call(
        functools.partial(stats_kernel, n),
        in_specs=[vmem, vmem],
        out_specs=[vmem, vmem],
        out_shape=[jax.ShapeDtypeStruct((n, 8, tok), F32), jax.ShapeDtypeStruct((8, 128), F32)],
        scratch_shapes=[
            pltpu.VMEM((n, 8, tok), F32),
            pltpu.VMEM((n, 8, tok), F32),
        ] + [pltpu.SemaphoreType.DMA((n,))] * 4,
        compiler_params=params(16, collective_id=0, has_side_effects=True),
        cost_estimate=cost(1e9, 2e6),
        name='stats',
    )(st, mask)


def grad_kernel(wt_ref, e_ref, cm_ref, gs_ref, lab_ref, g_ref, dx_ref):
    rows = wt_ref.shape[1]
    tok = e_ref.shape[2]
    index = lax.broadcasted_iota(jnp.int32, (CHUNK, tok), 0)
    for b in range(GROUP):
        m, over, scale = gs_ref[b, 0:1, :], gs_ref[b, 1:2, :], gs_ref[b, 2:3, :]
        for c in range(rows // CHUNK):
            sl = pl.ds(c * CHUNK, CHUNK)
            p = e_ref[b, sl, :] * (jnp.exp(cm_ref[b, c:c + 1, :] - m) * over)
            hit = index == lab_ref[b] - c * CHUNK
            g_ref[b, sl, :] = jnp.where(hit, p - scale, p).astype(BF16)
    dx = mm(wt_ref[...], side_by_side(g_ref), 1, 0)
    for b in range(GROUP):
        dx_ref[b] = dx[:, b * tok:(b + 1) * tok]


def grad(wt, e, cm, gs, lab):
    dim, rows = wt.shape
    n, _, tok = e.shape
    block = lambda r, c: pl.BlockSpec((GROUP, r, c), lambda i: (i, 0, 0))
    return pl.pallas_call(
        grad_kernel,
        grid=(n // GROUP,),
        in_specs=[pl.BlockSpec((dim, rows), lambda i: (0, 0)), block(rows, tok), block(8, tok), block(8, tok), block(1, tok)],
        out_specs=[block(rows, tok), block(dim, tok)],
        out_shape=[jax.ShapeDtypeStruct((n, rows, tok), BF16), jax.ShapeDtypeStruct((n, dim, tok), F32)],
        compiler_params=params(56),
        cost_estimate=cost(2 * n * tok * dim * rows, 6 * n * tok * rows),
        name='grad',
    )(wt, e, cm, gs, lab)


def head_kernel(x_ref, g_ref, out_ref):
    out_ref[...] = mm(side_by_side(x_ref), side_by_side(g_ref), 1, 1).astype(BF16)


def head(x, g):
    n, dim, tok = x.shape
    rows = g.shape[1]
    tile = 512
    return pl.pallas_call(
        head_kernel,
        grid=(rows // tile,),
        in_specs=[pl.BlockSpec((n, dim, tok), lambda i: (0, 0, 0)), pl.BlockSpec((n, tile, tok), lambda i: (0, i, 0))],
        out_specs=pl.BlockSpec((dim, tile), lambda i: (0, i)),
        out_shape=jax.ShapeDtypeStruct((dim, rows), BF16),
        compiler_params=params(56),
        cost_estimate=cost(2 * n * tok * dim * rows, 2 * n * tok * rows),
        name='head',
    )(x, g)


def solution(mesh):
    n = mesh.shape['stage']
    row_spec = P(('data', 'stage'), None)
    vocab_spec = P('stage', None)
    layer_spec = P('stage', None, None, None)
    acts_spec = P(('data', 'stage'), None, None)

    def per_device(x_loc, w_loc, labels, loss_mask, e_loc, next_ids, acts_loc, up_loc, down_loc):
        tok = x_loc.shape[0]
        offset = lax.axis_index('stage') * w_loc.shape[0]
        wt = w_loc.T
        x = lax.all_gather(x_loc.T, 'stage', axis=0)
        ids = (next_ids - offset).reshape(n, 1, tok)
        lab = (labels - offset).reshape(n, 1, tok)
        mask = loss_mask.astype(F32).reshape(n, 1, tok)
        embed_part = embed(ids, e_loc.T)
        embed_rows = lax.psum_scatter(embed_part, 'stage', scatter_dimension=0)
        stage_out = mlp(acts_loc[0].T, up_loc[0], jnp.swapaxes(down_loc[0], 1, 2))
        e, cm, st = logits(wt, x, lab)
        gs, loss = stats(st, mask)
        g, dx_part = grad(wt, e, cm, gs, lab)
        dx = lax.psum_scatter(dx_part, 'stage', scatter_dimension=0)
        dw = head(x, g)
        return loss[0, :1], dx.T, dw.T, embed_rows.T, stage_out.T[None]

    return jax.shard_map(
        per_device,
        mesh=mesh,
        in_specs=(row_spec, vocab_spec, P('data'), P('data'), vocab_spec, P('data'), acts_spec, layer_spec, layer_spec),
        out_specs=(P('data'), row_spec, row_spec, row_spec, acts_spec),
        check_vma=False,
    )
```

```python
import functools

import jax
import jax.numpy as jnp
from jax import lax
from jax.experimental import pallas as pl
from jax.experimental.pallas import tpu as pltpu
from jax.sharding import PartitionSpec as P

F32 = jnp.float32
BF16 = jnp.bfloat16
MESH = pl.DeviceIdType.MESH
CHUNK = 512
GROUP = 2
MIB = 1024 * 1024


def mm(a, b, ca, cb):
    return lax.dot_general(a, b, (((ca,), (cb,)), ((), ())), preferred_element_type=F32)


def params(limit, **kw):
    return pltpu.CompilerParams(vmem_limit_bytes=limit * MIB, **kw)


def cost(flops, nbytes):
    return pl.CostEstimate(flops=int(flops), bytes_accessed=int(nbytes), transcendentals=0)


def transpose_into(dst_ref, src, step):
    for c in range(0, src.shape[1], step):
        dst_ref[pl.ds(c, step), :] = src[:, c:c + step].T


def side_by_side(ref):
    return jnp.concatenate([ref[b] for b in range(ref.shape[0])], axis=1)


def gelu(x):
    k = 0.7978845608028654
    inner = x * (k + (k * 0.044715) * (x * x))
    half = 0.5 * x
    return half + half * jnp.tanh(inner)


def mlp_kernel(a_ref, up_ref, down_ref, y_ref, upt_ref):
    layers = up_ref.shape[0]
    stage = lax.axis_index('stage')
    middle = (stage > 0) & (stage < lax.axis_size('stage') - 1)

    @pl.when(pl.program_id(0) == 0)
    def _():
        for i in range(layers):
            transpose_into(upt_ref.at[i], up_ref[i], 256)

    @pl.when(middle)
    def _():
        h = a_ref[...]
        for i in range(layers):
            u = jnp.concatenate(
                [gelu(mm(upt_ref[i, pl.ds(c, 512), :], h, 1, 0)).astype(BF16) for c in range(0, up_ref.shape[2], 512)], axis=0)
            h = (h.astype(F32) + mm(down_ref[i], u, 1, 0)).astype(BF16)
        y_ref[...] = h

    @pl.when(jnp.logical_not(middle))
    def _():
        y_ref[...] = a_ref[...]


def mlp(at, up, down):
    dim, tokens = at.shape
    layers, _, hidden = up.shape
    tile = 512
    return pl.pallas_call(
        mlp_kernel,
        grid=(tokens // tile,),
        in_specs=[
            pl.BlockSpec((dim, tile), lambda i: (0, i)),
            pl.BlockSpec((layers, dim, hidden), lambda i: (0, 0, 0)),
            pl.BlockSpec((layers, dim, hidden), lambda i: (0, 0, 0)),
        ],
        out_specs=pl.BlockSpec((dim, tile), lambda i: (0, i)),
        out_shape=jax.ShapeDtypeStruct((dim, tokens), BF16),
        scratch_shapes=[pltpu.VMEM((layers, hidden, dim), BF16)],
        compiler_params=params(48),
        cost_estimate=cost(4 * layers * tokens * dim * hidden, 4 * tokens * dim + 4 * layers * dim * hidden),
        name='mlp',
    )(at, up, down)


def embed_kernel(ids_ref, et_ref, out_ref):
    rows = et_ref.shape[1]
    tok = ids_ref.shape[2]
    index = lax.broadcasted_iota(jnp.int32, (rows, GROUP * tok), 0)
    hot = jnp.where(index == side_by_side(ids_ref), 1.0, 0.0).astype(BF16)
    out = mm(et_ref[...], hot, 1, 0).astype(BF16)
    for b in range(GROUP):
        out_ref[b] = out[:, b * tok:(b + 1) * tok]


def embed(ids, et):
    n, _, tok = ids.shape
    dim, rows = et.shape
    return pl.pallas_call(
        embed_kernel,
        grid=(n // GROUP,),
        in_specs=[
            pl.BlockSpec((GROUP, 1, tok), lambda i: (i, 0, 0)),
            pl.BlockSpec((dim, rows), lambda i: (0, 0)),
        ],
        out_specs=pl.BlockSpec((GROUP, dim, tok), lambda i: (i, 0, 0)),
        out_shape=jax.ShapeDtypeStruct((n, dim, tok), BF16),
        compiler_params=params(48),
        cost_estimate=cost(2 * n * tok * dim * rows, 2 * dim * (n * tok + rows)),
        name='embed',
    )(ids, et)


def logits_kernel(wt_ref, x_ref, lab_ref, e_ref, cm_ref, st_ref, w_ref):
    rows = wt_ref.shape[1]
    tok = x_ref.shape[2]

    @pl.when(pl.program_id(0) == 0)
    def _():
        transpose_into(w_ref, wt_ref, 256)

    x = side_by_side(x_ref)
    lab = side_by_side(lab_ref)
    index = lax.broadcasted_iota(jnp.int32, (CHUNK, GROUP * tok), 0)
    maxes, sums = [], []
    target = jnp.zeros((1, GROUP * tok), F32)
    for c in range(rows // CHUNK):
        sl = pl.ds(c * CHUNK, CHUNK)
        z = mm(w_ref[sl, :], x, 1, 0)
        m = jnp.max(z, axis=0, keepdims=True)
        e = jnp.exp(z - m)
        for b in range(GROUP):
            e_ref[b, sl, :] = e[:, b * tok:(b + 1) * tok]
        maxes.append(m)
        sums.append(jnp.sum(e, axis=0, keepdims=True))
        target += jnp.sum(jnp.where(index == lab - c * CHUNK, z, 0.0), axis=0, keepdims=True)
    m = functools.reduce(jnp.maximum, maxes)
    s = sum(si * jnp.exp(mi - m) for mi, si in zip(maxes, sums))
    cm = jnp.concatenate(maxes + [jnp.zeros((8 - len(maxes), GROUP * tok), F32)], axis=0)
    st = jnp.concatenate([m, s, target, jnp.zeros((5, GROUP * tok), F32)], axis=0)
    for b in range(GROUP):
        cm_ref[b] = cm[:, b * tok:(b + 1) * tok]
        st_ref[b] = st[:, b * tok:(b + 1) * tok]


def logits(wt, x, lab):
    dim, rows = wt.shape
    n, _, tok = x.shape
    block = lambda r, c: pl.BlockSpec((GROUP, r, c), lambda i: (i, 0, 0))
    return pl.pallas_call(
        logits_kernel,
        grid=(n // GROUP,),
        in_specs=[pl.BlockSpec((dim, rows), lambda i: (0, 0)), block(dim, tok), block(1, tok)],
        out_specs=[block(rows, tok), block(8, tok), block(8, tok)],
        out_shape=[
            jax.ShapeDtypeStruct((n, rows, tok), F32),
            jax.ShapeDtypeStruct((n, 8, tok), F32),
            jax.ShapeDtypeStruct((n, 8, tok), F32),
        ],
        scratch_shapes=[pltpu.VMEM((rows, dim), BF16)],
        compiler_params=params(56),
        cost_estimate=cost(2 * n * tok * dim * rows, 4 * n * tok * rows),
        name='logits',
    )(wt, x, lab)


def stats_kernel(n, st_ref, mask_ref, out_ref, loss_ref, got, every, send1, recv1, send2, recv2):
    me = lax.axis_index('stage')
    barrier = pltpu.get_barrier_semaphore()
    peers = [lax.rem(me + d, n) for d in range(n)]
    for d in range(1, n):
        pl.semaphore_signal(barrier, inc=1, device_id={'stage': peers[d]}, device_id_type=MESH)
    pl.semaphore_wait(barrier, n - 1)

    first = []
    for d in range(1, n):
        first.append(pltpu.make_async_remote_copy(
            src_ref=st_ref.at[peers[d]], dst_ref=got.at[d], send_sem=send1.at[d], recv_sem=recv1.at[d],
            device_id={'stage': peers[d]}, device_id_type=MESH))
        first[-1].start()
    weight = mask_ref[...]
    count = jnp.maximum(jnp.sum(weight, keepdims=True)[0], 1.0)
    for copy in first:
        copy.wait()
    parts = [st_ref[me]] + [got[d] for d in range(1, n)]
    m = functools.reduce(jnp.maximum, [p[0:1] for p in parts])
    total = sum(p[1:2] * jnp.exp(p[0:1] - m) for p in parts)
    target = sum(p[2:3] for p in parts)
    w = mask_ref[me]
    scale = w / count
    term = w * (jnp.log(total) + m - target)
    mine = jnp.concatenate([m, scale / total, scale, term, jnp.zeros((4, m.shape[1]), F32)], axis=0)
    every[me] = mine
    second = []
    for d in range(1, n):
        second.append(pltpu.make_async_remote_copy(
            src_ref=every.at[me], dst_ref=every.at[me], send_sem=send2.at[d], recv_sem=recv2.at[d],
            device_id={'stage': peers[d]}, device_id_type=MESH))
        second[-1].start()
    for copy in second:
        copy.wait()
    out_ref[...] = every[...]
    loss_ref[...] = jnp.broadcast_to(jnp.sum(every[:, 3, :], keepdims=True) / count, loss_ref.shape)


def stats(st, mask):
    n, _, tok = st.shape
    vmem = pl.BlockSpec(memory_space=pltpu.VMEM)
    return pl.pallas_call(
        functools.partial(stats_kernel, n),
        in_specs=[vmem, vmem],
        out_specs=[vmem, vmem],
        out_shape=[jax.ShapeDtypeStruct((n, 8, tok), F32), jax.ShapeDtypeStruct((8, 128), F32)],
        scratch_shapes=[
            pltpu.VMEM((n, 8, tok), F32),
            pltpu.VMEM((n, 8, tok), F32),
        ] + [pltpu.SemaphoreType.DMA((n,))] * 4,
        compiler_params=params(16, collective_id=0, has_side_effects=True),
        cost_estimate=cost(1e9, 2e6),
        name='stats',
    )(st, mask)


def grad_kernel(n, e_hbm, w_hbm, x_hbm, cm_ref, gs_ref, lab_ref, dx_ref, dw_ref, w_buf, x_buf, e_buf, g_buf, send_buf, own, pair,
                chain, load_sem, e_sem, pair_send, pair_recv, chain_send, chain_recv):
    stage = lax.axis_index('stage')
    chips = n // 2
    far = chips // 2
    z, core = stage // 2, lax.rem(stage, 2)
    dim, tok = dx_ref.shape
    rows = w_buf.shape[1]
    half = dim // 2
    partner = {'stage': 2 * z + 1 - core}
    ahead = {'stage': 2 * lax.rem(z + 1, chips) + core}
    behind = {'stage': 2 * lax.rem(z + chips - 1, chips) + core}

    def chip_at(i):
        size = far - (i + 1) // 2
        sign = 2 * lax.rem(i, 2) - 1
        return lax.rem(z + sign * size + chips, chips)

    def block_at(i, own_side):
        return 2 * chip_at(i) + (core if own_side else 1 - core)

    def load_e(i, slot):
        return pltpu.make_async_copy(e_hbm.at[block_at(i, slot == 1)], e_buf.at[slot], e_sem.at[slot])

    for slot in range(2):
        load_e(0, slot).start()
    load_w = pltpu.make_async_copy(w_hbm, w_buf, load_sem.at[0])
    load_x = pltpu.make_async_copy(x_hbm, x_buf, load_sem.at[1])
    load_w.start()
    load_x.start()

    barrier = pltpu.get_barrier_semaphore()
    for peer in (partner, ahead, behind):
        pl.semaphore_signal(barrier, inc=1, device_id=peer, device_id_type=MESH)
    pl.semaphore_wait(barrier, 3)
    load_w.wait()

    index = lax.broadcasted_iota(jnp.int32, (CHUNK, tok), 0)

    def tile(slot, t, dst):
        gs, cm, lab = gs_ref[t], cm_ref[t], lab_ref[t]
        m, over, scale = gs[0:1], gs[1:2], gs[2:3]
        for c in range(rows // CHUNK):
            sl = pl.ds(c * CHUNK, CHUNK)
            p = e_buf[slot, sl, :] * (jnp.exp(cm[c:c + 1] - m) * over)
            g_buf[t, sl, :] = jnp.where(index == lab - c * CHUNK, p - scale, p).astype(BF16)
        dst[...] = mm(w_buf[...], g_buf[t], 1, 0)

    def pair_copy(i):
        return pltpu.make_async_remote_copy(
            src_ref=send_buf.at[lax.rem(i, 2)], dst_ref=pair.at[i], send_sem=pair_send.at[lax.rem(i, 2)],
            recv_sem=pair_recv.at[i], device_id=partner, device_id_type=MESH)

    def pair_add(i):
        pair_copy(i).wait_recv()
        own[i] += pair[i]

    def unit(way, k, h, src):
        sl = pl.ds(h * half, half)
        s = way * 8 + k * 2 + h
        return pltpu.make_async_remote_copy(
            src_ref=src.at[sl, :], dst_ref=chain.at[way * far + k, sl, :], send_sem=chain_send.at[s], recv_sem=chain_recv.at[s],
            device_id=ahead if way == 0 else behind, device_id_type=MESH)

    def place(way, k):
        return 0 if k == 0 else 2 * k - 1 + way

    def first_send(way):
        unit(way, 0, way, own.at[0]).start()

    def plain_send(way):
        unit(way, 1, 1 - way, own.at[place(way, 1)]).start()

    def forward(way, k, h):
        here = chain.at[way * far + k]
        unit(way, k, h, here).wait_recv()
        sl = pl.ds(h * half, half)
        here[sl, :] += own[place(way, k + 1), sl, :]
        unit(way, k + 1, h, here).start()

    def body(i, carry):
        load_e(i, 0).wait()

        @pl.when(i >= 2)
        def _():
            pair_copy(i - 2).wait_send()

        tile(0, block_at(i, False), send_buf.at[lax.rem(i, 2)])
        pair_copy(i).start()

        @pl.when(i < chips - 1)
        def _():
            load_e(i + 1, 0).start()

        load_e(i, 1).wait()
        tile(1, block_at(i, True), own.at[i])

        @pl.when(i < chips - 1)
        def _():
            load_e(i + 1, 1).start()

        @pl.when(i >= 1)
        def _():
            pair_add(i - 1)

        @pl.when(i == 1)
        def _():
            first_send(0)
            first_send(1)

        @pl.when(i == 2)
        def _():
            plain_send(0)

        @pl.when(i == 3)
        def _():
            plain_send(1)

        @pl.when(i == chips - 2)
        def _():
            for way in range(2):
                forward(way, 0, way)
        return carry

    lax.fori_loop(0, chips, body, 0)
    pair_add(chips - 1)
    for way in range(2):
        forward(way, 1, 1 - way)
    load_x.wait()
    width = dw_ref.shape[1] // 6

    def head(j, carry):
        for q in range(2):
            start = pl.multiple_of((2 * j + q) * width, width)
            g = jnp.concatenate([g_buf[b, pl.ds(start, width), :] for b in range(n)], axis=1)
            dw_ref[:, pl.ds(start, width)] = mm(side_by_side(x_buf), g, 1, 1).astype(BF16)
        for k in range(3):
            @pl.when(j == k)
            def _():
                for way in range(2):
                    if k == 0:
                        forward(way, 1, way)
                    if k == 1:
                        forward(way, 2, 1 - way)
                    if k == 2:
                        forward(way, 2, way)
        return carry

    lax.fori_loop(0, 3, head, 0)
    for h in range(2):
        for way in range(2):
            unit(way, far - 1, h, own.at[0]).wait_recv()
    dx_ref[...] = own[chips - 1] + (chain[far - 1] + chain[2 * far - 1])
    for i in range(chips - 2, chips):
        pair_copy(i).wait_send()
    for way in range(2):
        for k in range(far):
            for h in range(2):
                if k > 0 or h == way:
                    unit(way, k, h, own.at[0]).wait_send()


def grad(wt, e, x, cm, gs, lab):
    dim, rows = wt.shape
    n, _, tok = e.shape
    chips = n // 2
    vmem = pl.BlockSpec(memory_space=pltpu.VMEM)
    anywhere = pl.BlockSpec(memory_space=pl.ANY)
    return pl.pallas_call(
        functools.partial(grad_kernel, n),
        in_specs=[anywhere, anywhere, anywhere, vmem, vmem, vmem],
        out_specs=[vmem, vmem],
        out_shape=[jax.ShapeDtypeStruct((dim, tok), F32), jax.ShapeDtypeStruct((dim, rows), BF16)],
        scratch_shapes=[
            pltpu.VMEM((dim, rows), BF16),
            pltpu.VMEM((n, dim, tok), BF16),
            pltpu.VMEM((2, rows, tok), F32),
            pltpu.VMEM((n, rows, tok), BF16),
            pltpu.VMEM((2, dim, tok), F32),
            pltpu.VMEM((chips, dim, tok), F32),
            pltpu.VMEM((chips, dim, tok), F32),
            pltpu.VMEM((chips, dim, tok), F32),
            pltpu.SemaphoreType.DMA((2,)),
            pltpu.SemaphoreType.DMA((2,)),
            pltpu.SemaphoreType.DMA((2,)),
            pltpu.SemaphoreType.DMA((chips,)),
            pltpu.SemaphoreType.DMA((16,)),
            pltpu.SemaphoreType.DMA((16,)),
        ],
        compiler_params=pltpu.CompilerParams(vmem_limit_bytes=60 * MIB, collective_id=1, has_side_effects=True),
        cost_estimate=cost(4 * n * tok * dim * rows, 6 * n * tok * rows),
        name='grad',
    )(e, wt, x, cm, gs, lab)


def solution(mesh):
    n = mesh.shape['stage']
    row_spec = P(('data', 'stage'), None)
    vocab_spec = P('stage', None)
    layer_spec = P('stage', None, None, None)
    acts_spec = P(('data', 'stage'), None, None)

    def per_device(x_loc, w_loc, labels, loss_mask, e_loc, next_ids, acts_loc, up_loc, down_loc):
        tok = x_loc.shape[0]
        offset = lax.axis_index('stage') * w_loc.shape[0]
        wt = w_loc.T
        x = lax.all_gather(x_loc.T, 'stage', axis=0)
        ids = (next_ids - offset).reshape(n, 1, tok)
        lab = (labels - offset).reshape(n, 1, tok)
        mask = loss_mask.astype(F32).reshape(n, 1, tok)
        embed_part = embed(ids, e_loc.T)
        embed_rows = lax.psum_scatter(embed_part, 'stage', scatter_dimension=0)
        stage_out = mlp(acts_loc[0].T, up_loc[0], jnp.swapaxes(down_loc[0], 1, 2))
        lab, stage_out = lax.optimization_barrier((lab, stage_out))
        e, cm, st = logits(wt, x, lab)
        gs, loss = stats(st, mask)
        dx, dw = grad(wt, e, x, cm, gs, lab)
        return loss[0, :1], dx.T, dw.T, embed_rows.T, stage_out.T[None]

    return jax.shard_map(
        per_device,
        mesh=mesh,
        in_specs=(row_spec, vocab_spec, P('data'), P('data'), vocab_spec, P('data'), acts_spec, layer_spec, layer_spec),
        out_specs=(P('data'), row_spec, row_spec, row_spec, acts_spec),
        check_vma=False,
    )
```

```python
import functools

import jax
import jax.numpy as jnp
from jax import lax
from jax.experimental import pallas as pl
from jax.experimental.pallas import tpu as pltpu
from jax.sharding import PartitionSpec as P

F32 = jnp.float32
BF16 = jnp.bfloat16
MESH = pl.DeviceIdType.MESH
CHUNK = 512
GROUP = 2
MIB = 1024 * 1024


def mm(a, b, ca, cb):
    return lax.dot_general(a, b, (((ca,), (cb,)), ((), ())), preferred_element_type=F32)


def params(limit, **kw):
    return pltpu.CompilerParams(vmem_limit_bytes=limit * MIB, **kw)


def cost(flops, nbytes):
    return pl.CostEstimate(flops=int(flops), bytes_accessed=int(nbytes), transcendentals=0)


def transpose_into(dst_ref, src, step):
    for c in range(0, src.shape[1], step):
        dst_ref[pl.ds(c, step), :] = src[:, c:c + step].T


def side_by_side(ref):
    return jnp.concatenate([ref[b] for b in range(ref.shape[0])], axis=1)


def gelu(x):
    k = 0.7978845608028654
    inner = x * (k + (k * 0.044715) * (x * x))
    half = 0.5 * x
    return half + half * jnp.tanh(inner)


MLP_TILE = 512
MLP_FIRST = 4


def mlp_layers(h, upt_ref, down_ref):
    for i in range(upt_ref.shape[0]):
        u = jnp.concatenate(
            [gelu(mm(upt_ref[i, pl.ds(c, 512), :], h, 1, 0)).astype(BF16) for c in range(0, upt_ref.shape[1], 512)], axis=0)
        h = (h.astype(F32) + mm(down_ref[i], u, 1, 0)).astype(BF16)
    return h


def is_middle():
    stage = lax.axis_index('stage')
    return (stage > 0) & (stage < lax.axis_size('stage') - 1)


def mlp_kernel(a_ref, up_ref, down_ref, y_ref, upt_ref):
    @pl.when(pl.program_id(0) == 0)
    def _():
        for i in range(up_ref.shape[0]):
            transpose_into(upt_ref.at[i], up_ref[i], 256)

    @pl.when(is_middle())
    def _():
        y_ref[...] = mlp_layers(a_ref[...], upt_ref, down_ref)

    @pl.when(jnp.logical_not(is_middle()))
    def _():
        y_ref[...] = a_ref[...]


def mlp(at, up, down):
    dim = at.shape[0]
    layers, _, hidden = up.shape
    tokens = MLP_FIRST * MLP_TILE
    whole = lambda shape: pl.BlockSpec(shape, lambda i: (0, 0, 0))
    tile = pl.BlockSpec((dim, MLP_TILE), lambda i: (0, i))
    return pl.pallas_call(
        mlp_kernel,
        grid=(MLP_FIRST,),
        in_specs=[tile, whole((layers, dim, hidden)), whole((layers, dim, hidden))],
        out_specs=[tile, whole((layers, hidden, dim))],
        out_shape=[jax.ShapeDtypeStruct((dim, tokens), BF16), jax.ShapeDtypeStruct((layers, hidden, dim), BF16)],
        compiler_params=params(48),
        cost_estimate=cost(4 * layers * tokens * dim * hidden, 4 * tokens * dim + 4 * layers * dim * hidden),
        name='mlp',
    )(at, up, down)


def embed_kernel(ids_ref, et_ref, out_ref):
    rows = et_ref.shape[1]
    tok = ids_ref.shape[2]
    index = lax.broadcasted_iota(jnp.int32, (rows, GROUP * tok), 0)
    hot = jnp.where(index == side_by_side(ids_ref), 1.0, 0.0).astype(BF16)
    out = mm(et_ref[...], hot, 1, 0).astype(BF16)
    for b in range(GROUP):
        out_ref[b] = out[:, b * tok:(b + 1) * tok]


def embed(ids, et):
    n, _, tok = ids.shape
    dim, rows = et.shape
    return pl.pallas_call(
        embed_kernel,
        grid=(n // GROUP,),
        in_specs=[
            pl.BlockSpec((GROUP, 1, tok), lambda i: (i, 0, 0)),
            pl.BlockSpec((dim, rows), lambda i: (0, 0)),
        ],
        out_specs=pl.BlockSpec((GROUP, dim, tok), lambda i: (i, 0, 0)),
        out_shape=jax.ShapeDtypeStruct((n, dim, tok), BF16),
        compiler_params=params(48),
        cost_estimate=cost(2 * n * tok * dim * rows, 2 * dim * (n * tok + rows)),
        name='embed',
    )(ids, et)


def logits_kernel(wt_ref, x_ref, lab_ref, e_ref, cm_ref, st_ref, w_ref):
    rows = wt_ref.shape[1]
    tok = x_ref.shape[2]

    @pl.when(pl.program_id(0) == 0)
    def _():
        transpose_into(w_ref, wt_ref, 256)

    x = side_by_side(x_ref)
    lab = side_by_side(lab_ref)
    index = lax.broadcasted_iota(jnp.int32, (CHUNK, GROUP * tok), 0)
    maxes, sums = [], []
    target = jnp.zeros((1, GROUP * tok), F32)
    for c in range(rows // CHUNK):
        sl = pl.ds(c * CHUNK, CHUNK)
        z = mm(w_ref[sl, :], x, 1, 0)
        m = jnp.max(z, axis=0, keepdims=True)
        e = jnp.exp(z - m)
        for b in range(GROUP):
            e_ref[b, sl, :] = e[:, b * tok:(b + 1) * tok]
        maxes.append(m)
        sums.append(jnp.sum(e, axis=0, keepdims=True))
        target += jnp.sum(jnp.where(index == lab - c * CHUNK, z, 0.0), axis=0, keepdims=True)
    m = functools.reduce(jnp.maximum, maxes)
    s = sum(si * jnp.exp(mi - m) for mi, si in zip(maxes, sums))
    cm = jnp.concatenate(maxes + [jnp.zeros((8 - len(maxes), GROUP * tok), F32)], axis=0)
    st = jnp.concatenate([m, s, target, jnp.zeros((5, GROUP * tok), F32)], axis=0)
    for b in range(GROUP):
        cm_ref[b] = cm[:, b * tok:(b + 1) * tok]
        st_ref[b] = st[:, b * tok:(b + 1) * tok]


def logits(wt, x, lab):
    dim, rows = wt.shape
    n, _, tok = x.shape
    block = lambda r, c: pl.BlockSpec((GROUP, r, c), lambda i: (i, 0, 0))
    return pl.pallas_call(
        logits_kernel,
        grid=(n // GROUP,),
        in_specs=[pl.BlockSpec((dim, rows), lambda i: (0, 0)), block(dim, tok), block(1, tok)],
        out_specs=[block(rows, tok), block(8, tok), block(8, tok)],
        out_shape=[
            jax.ShapeDtypeStruct((n, rows, tok), F32),
            jax.ShapeDtypeStruct((n, 8, tok), F32),
            jax.ShapeDtypeStruct((n, 8, tok), F32),
        ],
        scratch_shapes=[pltpu.VMEM((rows, dim), BF16)],
        compiler_params=params(56),
        cost_estimate=cost(2 * n * tok * dim * rows, 4 * n * tok * rows),
        name='logits',
    )(wt, x, lab)


def stats_kernel(n, st_ref, mask_ref, out_ref, loss_ref, got, every, send1, recv1, send2, recv2):
    me = lax.axis_index('stage')
    barrier = pltpu.get_barrier_semaphore()
    peers = [lax.rem(me + d, n) for d in range(n)]
    for d in range(1, n):
        pl.semaphore_signal(barrier, inc=1, device_id={'stage': peers[d]}, device_id_type=MESH)
    pl.semaphore_wait(barrier, n - 1)

    first = []
    for d in range(1, n):
        first.append(pltpu.make_async_remote_copy(
            src_ref=st_ref.at[peers[d]], dst_ref=got.at[d], send_sem=send1.at[d], recv_sem=recv1.at[d],
            device_id={'stage': peers[d]}, device_id_type=MESH))
        first[-1].start()
    weight = mask_ref[...]
    count = jnp.maximum(jnp.sum(weight, keepdims=True)[0], 1.0)
    for copy in first:
        copy.wait()
    parts = [st_ref[me]] + [got[d] for d in range(1, n)]
    m = functools.reduce(jnp.maximum, [p[0:1] for p in parts])
    total = sum(p[1:2] * jnp.exp(p[0:1] - m) for p in parts)
    target = sum(p[2:3] for p in parts)
    w = mask_ref[me]
    scale = w / count
    term = w * (jnp.log(total) + m - target)
    mine = jnp.concatenate([m, scale / total, scale, term, jnp.zeros((4, m.shape[1]), F32)], axis=0)
    every[me] = mine
    second = []
    for d in range(1, n):
        second.append(pltpu.make_async_remote_copy(
            src_ref=every.at[me], dst_ref=every.at[me], send_sem=send2.at[d], recv_sem=recv2.at[d],
            device_id={'stage': peers[d]}, device_id_type=MESH))
        second[-1].start()
    for copy in second:
        copy.wait()
    out_ref[...] = every[...]
    loss_ref[...] = jnp.broadcast_to(jnp.sum(every[:, 3, :], keepdims=True) / count, loss_ref.shape)


def stats(st, mask):
    n, _, tok = st.shape
    vmem = pl.BlockSpec(memory_space=pltpu.VMEM)
    return pl.pallas_call(
        functools.partial(stats_kernel, n),
        in_specs=[vmem, vmem],
        out_specs=[vmem, vmem],
        out_shape=[jax.ShapeDtypeStruct((n, 8, tok), F32), jax.ShapeDtypeStruct((8, 128), F32)],
        scratch_shapes=[
            pltpu.VMEM((n, 8, tok), F32),
            pltpu.VMEM((n, 8, tok), F32),
        ] + [pltpu.SemaphoreType.DMA((n,))] * 4,
        compiler_params=params(16, collective_id=0, has_side_effects=True),
        cost_estimate=cost(1e9, 2e6),
        name='stats',
    )(st, mask)


def grad_kernel(n, e_hbm, w_hbm, x_hbm, a_hbm, upt_hbm, down_hbm, cm_ref, gs_ref, lab_ref, dx_ref, dw_hbm, y_hbm, g_buf, send_buf,
                own, pair, chain, load_sem, e_sem, pair_send, pair_recv, chain_send, chain_recv, a_sem, y_sem):
    stage = lax.axis_index('stage')
    chips = n // 2
    far = chips // 2
    z, core = stage // 2, lax.rem(stage, 2)
    dim, tok = dx_ref.shape
    rows = w_hbm.shape[1]
    half = dim // 2
    partner = {'stage': 2 * z + 1 - core}
    ahead = {'stage': 2 * lax.rem(z + 1, chips) + core}
    behind = {'stage': 2 * lax.rem(z + chips - 1, chips) + core}

    def chip_at(i):
        size = far - (i + 1) // 2
        sign = 2 * lax.rem(i, 2) - 1
        return lax.rem(z + sign * size + chips, chips)

    def block_at(i, own_side):
        return 2 * chip_at(i) + (core if own_side else 1 - core)

    barrier = pltpu.get_barrier_semaphore()
    for peer in (partner, ahead, behind):
        pl.semaphore_signal(barrier, inc=1, device_id=peer, device_id_type=MESH)
    pl.semaphore_wait(barrier, 3)

    def pair_copy(i):
        return pltpu.make_async_remote_copy(
            src_ref=send_buf.at[lax.rem(i, 2)], dst_ref=pair.at[i], send_sem=pair_send.at[lax.rem(i, 2)],
            recv_sem=pair_recv.at[i], device_id=partner, device_id_type=MESH)

    def pair_add(i):
        pair_copy(i).wait_recv()
        own[i] += pair[i]

    def unit(way, k, h, src):
        sl = pl.ds(h * half, half)
        s = way * 8 + k * 2 + h
        return pltpu.make_async_remote_copy(
            src_ref=src.at[sl, :], dst_ref=chain.at[way * far + k, sl, :], send_sem=chain_send.at[s], recv_sem=chain_recv.at[s],
            device_id=ahead if way == 0 else behind, device_id_type=MESH)

    def place(way, k):
        return 0 if k == 0 else 2 * k - 1 + way

    def first_send(way):
        unit(way, 0, way, own.at[0]).start()

    def plain_send(way):
        unit(way, 1, 1 - way, own.at[place(way, 1)]).start()

    def forward(way, k, h):
        here = chain.at[way * far + k]
        unit(way, k, h, here).wait_recv()
        sl = pl.ds(h * half, half)
        here[sl, :] += own[place(way, k + 1), sl, :]
        unit(way, k + 1, h, here).start()

    def gradients(w_buf, e_buf):
        def load_e(i, q):
            slot = lax.rem(i, 2)
            return pltpu.make_async_copy(e_hbm.at[block_at(i, q == 1)], e_buf.at[slot, q], e_sem.at[slot, q])

        for q in range(2):
            load_e(0, q).start()
        load_w = pltpu.make_async_copy(w_hbm, w_buf, load_sem.at[0])
        load_w.start()
        index = lax.broadcasted_iota(jnp.int32, (CHUNK, tok), 0)
        load_w.wait()

        def body(i, carry):
            @pl.when(i < chips - 1)
            def _():
                for q in range(2):
                    load_e(i + 1, q).start()

            @pl.when(i >= 2)
            def _():
                pair_copy(i - 2).wait_send()

            for q in range(2):
                load_e(i, q).wait()
            slot = lax.rem(i, 2)
            blocks = [block_at(i, q == 1) for q in range(2)]
            parts = [[], []]
            for q in range(2):
                gs, cm, lab = gs_ref[blocks[q]], cm_ref[blocks[q]], lab_ref[blocks[q]]
                m, over, scale = gs[0:1], gs[1:2], gs[2:3]
                for c in range(rows // CHUNK):
                    sl = pl.ds(c * CHUNK, CHUNK)
                    p = e_buf[slot, q, sl, :] * (jnp.exp(cm[c:c + 1] - m) * over)
                    g = jnp.where(index == lab - c * CHUNK, p - scale, p).astype(BF16)
                    g_buf[blocks[q], sl, :] = g
                    parts[q].append(g)
            both = jnp.concatenate([jnp.concatenate(p, axis=0) for p in parts], axis=1)
            dx = mm(w_buf[...], both, 1, 0)
            send_buf[slot] = dx[:, :tok]
            own[i] = dx[:, tok:]
            pair_copy(i).start()

            @pl.when(i >= 1)
            def _():
                pair_add(i - 1)

            @pl.when(i == 1)
            def _():
                first_send(0)
                first_send(1)

            @pl.when(i == 2)
            def _():
                plain_send(0)

            @pl.when(i == 3)
            def _():
                plain_send(1)

            @pl.when(i == chips - 2)
            def _():
                for way in range(2):
                    forward(way, 0, way)
            return carry

        lax.fori_loop(0, chips, body, 0)

    pl.run_scoped(gradients, pltpu.VMEM((dim, rows), BF16), pltpu.VMEM((2, 2, rows, tok), F32))
    pair_add(chips - 1)

    def fill(x_buf, upt_buf, down_buf, a_buf, y_buf, dw_buf):
        loads = [
            pltpu.make_async_copy(src, dst, load_sem.at[k])
            for k, (src, dst) in enumerate([(x_hbm, x_buf), (upt_hbm, upt_buf), (down_hbm, down_buf)])
        ]
        for load in loads:
            load.start()
        tiles = y_hbm.shape[1] // MLP_TILE

        def cols(m):
            return pl.ds(pl.multiple_of(m * MLP_TILE, MLP_TILE), MLP_TILE)

        def load_a(m):
            slot = lax.rem(m, 2)
            return pltpu.make_async_copy(a_hbm.at[:, cols(m + MLP_FIRST)], a_buf.at[slot], a_sem.at[slot])

        def store_y(m):
            slot = lax.rem(m, 2)
            return pltpu.make_async_copy(y_buf.at[slot], y_hbm.at[:, cols(m)], y_sem.at[slot])

        load_a(0).start()
        loads[0].wait()
        width = 512
        pieces = rows // width

        def store_dw(j):
            slot = lax.rem(j, 2)
            start = pl.multiple_of(j * width, width)
            return pltpu.make_async_copy(dw_buf.at[slot], dw_hbm.at[:, pl.ds(start, width)], y_sem.at[slot])

        def head(j, carry):
            start = pl.multiple_of(j * width, width)
            g = jnp.concatenate([g_buf[b, pl.ds(start, width), :] for b in range(n)], axis=1)

            @pl.when(j >= 2)
            def _():
                store_dw(j - 2).wait()

            dw_buf[lax.rem(j, 2)] = mm(side_by_side(x_buf), g, 1, 1).astype(BF16)
            store_dw(j).start()

            @pl.when(j == 0)
            def _():
                for way in range(2):
                    forward(way, 1, 1 - way)

            @pl.when(j == 2)
            def _():
                for way in range(2):
                    forward(way, 1, way)

            @pl.when(j == 4)
            def _():
                for way in range(2):
                    forward(way, 2, 1 - way)
            return carry

        lax.fori_loop(0, pieces, head, 0)
        for j in range(pieces - 2, pieces):
            store_dw(j).wait()
        loads[1].wait()
        loads[2].wait()

        def layers(m, carry):
            slot = lax.rem(m, 2)

            @pl.when(m < tiles - 1)
            def _():
                load_a(m + 1).start()

            load_a(m).wait()

            @pl.when(m >= 2)
            def _():
                store_y(m - 2).wait()

            @pl.when(is_middle())
            def _():
                y_buf[slot] = mlp_layers(a_buf[slot], upt_buf, down_buf)

            @pl.when(jnp.logical_not(is_middle()))
            def _():
                y_buf[slot] = a_buf[slot]

            store_y(m).start()

            @pl.when(m == 0)
            def _():
                for way in range(2):
                    forward(way, 2, way)
            return carry

        lax.fori_loop(0, tiles, layers, 0)
        for m in range(tiles - 2, tiles):
            store_y(m).wait()

    pl.run_scoped(
        fill, pltpu.VMEM(x_hbm.shape, BF16), pltpu.VMEM(upt_hbm.shape, BF16), pltpu.VMEM(down_hbm.shape, BF16),
        pltpu.VMEM((2, dim, MLP_TILE), BF16), pltpu.VMEM((2, dim, MLP_TILE), BF16), pltpu.VMEM((2, dim, 512), BF16))
    for h in range(2):
        for way in range(2):
            unit(way, far - 1, h, own.at[0]).wait_recv()
    dx_ref[...] = own[chips - 1] + (chain[far - 1] + chain[2 * far - 1])
    for i in range(chips - 2, chips):
        pair_copy(i).wait_send()
    for way in range(2):
        for k in range(far):
            for h in range(2):
                if k > 0 or h == way:
                    unit(way, k, h, own.at[0]).wait_send()


def grad(wt, e, x, at, upt, down, cm, gs, lab):
    dim, rows = wt.shape
    n, _, tok = e.shape
    chips = n // 2
    tokens = at.shape[1] - MLP_FIRST * MLP_TILE
    vmem = pl.BlockSpec(memory_space=pltpu.VMEM)
    anywhere = pl.BlockSpec(memory_space=pl.ANY)
    dma = pltpu.SemaphoreType.DMA
    return pl.pallas_call(
        functools.partial(grad_kernel, n),
        in_specs=[anywhere] * 6 + [vmem] * 3,
        out_specs=[vmem, anywhere, anywhere],
        out_shape=[
            jax.ShapeDtypeStruct((dim, tok), F32),
            jax.ShapeDtypeStruct((dim, rows), BF16),
            jax.ShapeDtypeStruct((dim, tokens), BF16),
        ],
        scratch_shapes=[
            pltpu.VMEM((n, rows, tok), BF16),
            pltpu.VMEM((2, dim, tok), F32),
            pltpu.VMEM((chips, dim, tok), F32),
            pltpu.VMEM((chips, dim, tok), F32),
            pltpu.VMEM((chips, dim, tok), F32),
            dma((3,)), dma((2, 2)), dma((2,)), dma((chips,)), dma((16,)), dma((16,)), dma((2,)), dma((2,)),
        ],
        compiler_params=pltpu.CompilerParams(vmem_limit_bytes=63 * MIB, collective_id=1, has_side_effects=True),
        cost_estimate=cost(6 * n * tok * dim * rows, 6 * n * tok * rows),
        name='grad',
    )(e, wt, x, at, upt, down, cm, gs, lab)


def solution(mesh):
    n = mesh.shape['stage']
    row_spec = P(('data', 'stage'), None)
    vocab_spec = P('stage', None)
    layer_spec = P('stage', None, None, None)
    acts_spec = P(('data', 'stage'), None, None)

    def per_device(x_loc, w_loc, labels, loss_mask, e_loc, next_ids, acts_loc, up_loc, down_loc):
        tok = x_loc.shape[0]
        offset = lax.axis_index('stage') * w_loc.shape[0]
        wt = w_loc.T
        x = lax.all_gather(x_loc.T, 'stage', axis=0)
        ids = (next_ids - offset).reshape(n, 1, tok)
        lab = (labels - offset).reshape(n, 1, tok)
        mask = loss_mask.astype(F32).reshape(n, 1, tok)
        embed_part = embed(ids, e_loc.T)
        embed_rows = lax.psum_scatter(embed_part, 'stage', scatter_dimension=0)
        at, down = acts_loc[0].T, jnp.swapaxes(down_loc[0], 1, 2)
        y0, upt = mlp(at, up_loc[0], down)
        lab, y0 = lax.optimization_barrier((lab, y0))
        e, cm, st = logits(wt, x, lab)
        gs, loss = stats(st, mask)
        dx, dw, y1 = grad(wt, e, x, at, upt, down, cm, gs, lab)
        stage_out = jnp.concatenate([y0, y1], axis=1)
        return loss[0, :1], dx.T, dw.T, embed_rows.T, stage_out.T[None]

    return jax.shard_map(
        per_device,
        mesh=mesh,
        in_specs=(row_spec, vocab_spec, P('data'), P('data'), vocab_spec, P('data'), acts_spec, layer_spec, layer_spec),
        out_specs=(P('data'), row_spec, row_spec, row_spec, acts_spec),
        check_vma=False,
    )
```

```python
import functools

import jax
import jax.numpy as jnp
from jax import lax
from jax.experimental import pallas as pl
from jax.experimental.pallas import tpu as pltpu
from jax.sharding import PartitionSpec as P

F32 = jnp.float32
BF16 = jnp.bfloat16
MESH = pl.DeviceIdType.MESH
CHUNK = 512
GROUP = 2
MIB = 1024 * 1024


def mm(a, b, ca, cb):
    return lax.dot_general(a, b, (((ca,), (cb,)), ((), ())), preferred_element_type=F32)


def params(limit, **kw):
    return pltpu.CompilerParams(vmem_limit_bytes=limit * MIB, **kw)


def cost(flops, nbytes):
    return pl.CostEstimate(flops=int(flops), bytes_accessed=int(nbytes), transcendentals=0)


def transpose_into(dst_ref, src, step):
    for c in range(0, src.shape[1], step):
        dst_ref[pl.ds(c, step), :] = src[:, c:c + step].T


def side_by_side(ref):
    return jnp.concatenate([ref[b] for b in range(ref.shape[0])], axis=1)


def gelu(x):
    k = 0.7978845608028654
    inner = x * (k + (k * 0.044715) * (x * x))
    half = 0.5 * x
    return half + half * jnp.tanh(inner)


MLP_TILE = 512
MLP_GATHER = 1
MLP_STATS = 5


def mlp_layer(h, upt, down):
    hidden = upt.shape[0]
    u = jnp.concatenate(
        [gelu(mm(upt[pl.ds(c, 512), :], h, 1, 0)).astype(BF16) for c in range(0, hidden, 512)], axis=0)
    return (h.astype(F32) + mm(down[...], u, 1, 0)).astype(BF16)


def is_middle():
    stage = lax.axis_index('stage')
    return (stage > 0) & (stage < lax.axis_size('stage') - 1)


def mlp_step(src, dst, upt, down):
    @pl.when(is_middle())
    def _():
        dst[...] = mlp_layer(src[...], upt, down)

    @pl.when(jnp.logical_not(is_middle()))
    def _():
        dst[...] = src[...]


class Place:
    def __init__(self, n):
        stage = lax.axis_index('stage')
        self.chips = n // 2
        self.far = self.chips // 2
        self.z, self.core = stage // 2, lax.rem(stage, 2)
        self.partner = {'stage': 2 * self.z + 1 - self.core}
        self.along = [{'stage': 2 * self.chip(1) + self.core}, {'stage': 2 * self.chip(-1) + self.core}]

    def chip(self, steps):
        return lax.rem(self.z + steps + self.chips, self.chips)

    def block(self, chip, own_side):
        return 2 * chip + (self.core if own_side else 1 - self.core)

    def greet(self, barrier):
        for peer in [self.partner] + self.along:
            pl.semaphore_signal(barrier, inc=1, device_id=peer, device_id_type=MESH)
        pl.semaphore_wait(barrier, 3)


def gather_kernel(n, x_ref, ids_ref, et_hbm, up_hbm, down_hbm, a_hbm, x_out, h_out, y_out, upt_out, x_all, et, up_buf, upt_buf,
                  down_buf, a_buf, y_buf, send_buf, own, pair, load_sem, out_sem, ring_send, ring_recv, side_send, side_recv,
                  pair_send, pair_recv):
    here = Place(n)
    dim, tok = x_ref.shape
    half = dim // 2
    rows = et.shape[1]
    layers = up_buf.shape[0]
    mine = here.block(here.z, True)
    loads = [
        pltpu.make_async_copy(src, dst, load_sem.at[k])
        for k, (src, dst) in enumerate([
            (et_hbm, et), (up_hbm, up_buf), (down_hbm, down_buf), (a_hbm.at[:, pl.ds(0, MLP_TILE)], a_buf), (x_ref, x_all.at[mine])])
    ]
    for load in loads:
        load.start()
    here.greet(pltpu.get_barrier_semaphore())

    def unit(way, k, h):
        sl = pl.ds(h * half, half)
        block = here.block(here.chip(k if way else -k), True)
        src = x_ref.at[sl, :] if k == 0 else x_all.at[block, sl, :]
        s = way * 8 + k * 2 + h
        return pltpu.make_async_remote_copy(
            src_ref=src, dst_ref=x_all.at[block, sl, :], send_sem=ring_send.at[s], recv_sem=ring_recv.at[s],
            device_id=here.along[way], device_id_type=MESH)

    def side(way, k, h):
        sl = pl.ds(h * half, half)
        block = here.block(here.chip(1 + k if way else -1 - k), True)
        s = way * 8 + k * 2 + h
        return pltpu.make_async_remote_copy(
            src_ref=x_all.at[block, sl, :], dst_ref=x_all.at[block, sl, :], send_sem=side_send.at[s], recv_sem=side_recv.at[s],
            device_id=here.partner, device_id_type=MESH)

    def side_mine():
        return pltpu.make_async_remote_copy(
            src_ref=x_ref, dst_ref=x_all.at[mine], send_sem=side_send.at[16], recv_sem=side_recv.at[16],
            device_id=here.partner, device_id_type=MESH)

    last = here.far - 1
    arrivals = [[(k, h) for k in range(last) for h in range(2)] + [(last, way)] for way in range(2)]

    def event(u):
        for way in range(2):
            k, h = arrivals[way][u]
            unit(way, k, h).wait_recv()
            if (k + 1, h) in arrivals[way]:
                unit(way, k + 1, h).start()
            side(way, k, h).start()

    for h in range(2):
        for way in range(2):
            unit(way, 0, h).start()
    side_mine().start()

    def pair_copy(i):
        return pltpu.make_async_remote_copy(
            src_ref=send_buf.at[lax.rem(i, 2)], dst_ref=pair.at[i], send_sem=pair_send.at[lax.rem(i, 2)],
            recv_sem=pair_recv.at[i], device_id=here.partner, device_id_type=MESH)

    def pair_add(i):
        pair_copy(i).wait_recv()
        own[i] = (own[i].astype(F32) + pair[i].astype(F32)).astype(BF16)

    loads[0].wait()
    index = lax.broadcasted_iota(jnp.int32, (rows, 2 * tok), 0)

    def embed(i, carry):
        @pl.when(i >= 2)
        def _():
            pair_copy(i - 2).wait_send()

        ids = jnp.concatenate([ids_ref[here.block(i, False)], ids_ref[here.block(i, True)]], axis=1)
        hot = jnp.where(index == ids, 1.0, 0.0).astype(BF16)
        out = mm(et[...], hot, 1, 0).astype(BF16)
        send_buf[lax.rem(i, 2)] = out[:, :tok]
        own[i] = out[:, tok:]
        pair_copy(i).start()

        @pl.when(i >= 1)
        def _():
            pair_add(i - 1)

        for u in range(here.chips - 2):
            @pl.when(i == u + 2)
            def _():
                event(u)
        return carry

    lax.fori_loop(0, here.chips, embed, 0)
    loads[1].wait()
    for i in range(layers):
        transpose_into(upt_buf.at[i], up_buf[i], 256)
    loads[2].wait()
    loads[3].wait()
    mlp_step(a_buf, y_buf, upt_buf.at[0], down_buf.at[0])
    event(here.chips - 2)
    pair_add(here.chips - 1)
    outs = [
        pltpu.make_async_copy(src, dst, out_sem.at[k])
        for k, (src, dst) in enumerate([(own, h_out), (upt_buf, upt_out), (x_all, x_out), (y_buf, y_out)])
    ]
    outs[0].start()
    outs[1].start()
    loads[4].wait()
    side_mine().wait()
    for way in range(2):
        for k, h in arrivals[way]:
            side(way, k, h).wait()
    outs[2].start()
    for i in range(1, layers):
        mlp_step(y_buf, y_buf, upt_buf.at[i], down_buf.at[i])
    outs[3].start()
    for way in range(2):
        for k, h in arrivals[way]:
            unit(way, k, h).wait_send()
    for i in range(here.chips - 2, here.chips):
        pair_copy(i).wait_send()
    for out in outs:
        out.wait()


def gather(xt, ids, et, up, down, at):
    dim, tok = xt.shape
    n = ids.shape[0]
    rows = et.shape[1]
    layers, _, hidden = up.shape
    tokens = MLP_GATHER * MLP_TILE
    vmem = pl.BlockSpec(memory_space=pltpu.VMEM)
    anywhere = pl.BlockSpec(memory_space=pl.ANY)
    dma = pltpu.SemaphoreType.DMA
    return pl.pallas_call(
        functools.partial(gather_kernel, n),
        in_specs=[vmem, vmem] + [anywhere] * 4,
        out_specs=[anywhere] * 4,
        out_shape=[
            jax.ShapeDtypeStruct((n, dim, tok), BF16),
            jax.ShapeDtypeStruct((n // 2, dim, tok), BF16),
            jax.ShapeDtypeStruct((dim, tokens), BF16),
            jax.ShapeDtypeStruct((layers, hidden, dim), BF16),
        ],
        scratch_shapes=[
            pltpu.VMEM((n, dim, tok), BF16),
            pltpu.VMEM((dim, rows), BF16),
            pltpu.VMEM((layers, dim, hidden), BF16),
            pltpu.VMEM((layers, hidden, dim), BF16),
            pltpu.VMEM((layers, dim, hidden), BF16),
            pltpu.VMEM((dim, tokens), BF16),
            pltpu.VMEM((dim, tokens), BF16),
            pltpu.VMEM((2, dim, tok), BF16),
            pltpu.VMEM((n // 2, dim, tok), BF16),
            pltpu.VMEM((n // 2, dim, tok), BF16),
            dma((5,)), dma((4,)), dma((16,)), dma((16,)), dma((17,)), dma((17,)), dma((2,)), dma((n // 2,)),
        ],
        compiler_params=params(56, collective_id=2, has_side_effects=True),
        cost_estimate=cost(2 * n * tok * dim * rows, 4 * n * tok * dim),
        name='gather',
    )(xt, ids, et, up, down, at)


def logits_kernel(wt_ref, x_ref, lab_ref, e_ref, cm_ref, st_ref, w_ref):
    rows = wt_ref.shape[1]
    tok = x_ref.shape[2]

    @pl.when(pl.program_id(0) == 0)
    def _():
        transpose_into(w_ref, wt_ref, 256)

    x = side_by_side(x_ref)
    lab = side_by_side(lab_ref)
    index = lax.broadcasted_iota(jnp.int32, (CHUNK, GROUP * tok), 0)
    maxes, sums = [], []
    target = jnp.zeros((1, GROUP * tok), F32)
    for c in range(rows // CHUNK):
        sl = pl.ds(c * CHUNK, CHUNK)
        z = mm(w_ref[sl, :], x, 1, 0)
        m = jnp.max(z, axis=0, keepdims=True)
        e = jnp.exp(z - m)
        for b in range(GROUP):
            e_ref[b, sl, :] = e[:, b * tok:(b + 1) * tok]
        maxes.append(m)
        sums.append(jnp.sum(e, axis=0, keepdims=True))
        target += jnp.sum(jnp.where(index == lab - c * CHUNK, z, 0.0), axis=0, keepdims=True)
    m = functools.reduce(jnp.maximum, maxes)
    s = sum(si * jnp.exp(mi - m) for mi, si in zip(maxes, sums))
    cm = jnp.concatenate(maxes + [jnp.zeros((8 - len(maxes), GROUP * tok), F32)], axis=0)
    st = jnp.concatenate([m, s, target, jnp.zeros((5, GROUP * tok), F32)], axis=0)
    for b in range(GROUP):
        cm_ref[b] = cm[:, b * tok:(b + 1) * tok]
        st_ref[b] = st[:, b * tok:(b + 1) * tok]


def logits(wt, x, lab):
    dim, rows = wt.shape
    n, _, tok = x.shape
    block = lambda r, c: pl.BlockSpec((GROUP, r, c), lambda i: (i, 0, 0))
    return pl.pallas_call(
        logits_kernel,
        grid=(n // GROUP,),
        in_specs=[pl.BlockSpec((dim, rows), lambda i: (0, 0)), block(dim, tok), block(1, tok)],
        out_specs=[block(rows, tok), block(8, tok), block(8, tok)],
        out_shape=[
            jax.ShapeDtypeStruct((n, rows, tok), F32),
            jax.ShapeDtypeStruct((n, 8, tok), F32),
            jax.ShapeDtypeStruct((n, 8, tok), F32),
        ],
        scratch_shapes=[pltpu.VMEM((rows, dim), BF16)],
        compiler_params=params(56),
        cost_estimate=cost(2 * n * tok * dim * rows, 4 * n * tok * rows),
        name='logits',
    )(wt, x, lab)


def stats_kernel(n, st_ref, mask_ref, h_hbm, a_hbm, upt_hbm, down_hbm, out_ref, loss_ref, h_ref, y_hbm, got, every, own, chain,
                 upt_buf, down_buf, a_buf, y_buf, send1, recv1, send2, recv2, load_sem, chain_send, chain_recv, a_sem, y_sem):
    here = Place(n)
    me = lax.axis_index('stage')
    dim = h_ref.shape[0]
    half = dim // 2
    far = here.far
    layers = upt_buf.shape[0]
    loads = [
        pltpu.make_async_copy(src, dst, load_sem.at[k])
        for k, (src, dst) in enumerate([(h_hbm, own), (upt_hbm, upt_buf), (down_hbm, down_buf)])
    ]
    for load in loads:
        load.start()

    def load_a(m):
        start = pl.multiple_of((m + MLP_GATHER) * MLP_TILE, MLP_TILE)
        slot = lax.rem(m, 2)
        return pltpu.make_async_copy(a_hbm.at[:, pl.ds(start, MLP_TILE)], a_buf.at[slot], a_sem.at[slot])

    def store_y(m):
        slot = lax.rem(m, 2)
        start = pl.multiple_of(m * MLP_TILE, MLP_TILE)
        return pltpu.make_async_copy(y_buf.at[slot], y_hbm.at[:, pl.ds(start, MLP_TILE)], y_sem.at[slot])

    load_a(0).start()
    barrier = pltpu.get_barrier_semaphore()
    peers = [lax.rem(me + d, n) for d in range(n)]
    for d in range(1, n):
        pl.semaphore_signal(barrier, inc=1, device_id={'stage': peers[d]}, device_id_type=MESH)
    pl.semaphore_wait(barrier, n - 1)

    first = []
    for d in range(1, n):
        first.append(pltpu.make_async_remote_copy(
            src_ref=st_ref.at[peers[d]], dst_ref=got.at[d], send_sem=send1.at[d], recv_sem=recv1.at[d],
            device_id={'stage': peers[d]}, device_id_type=MESH))
        first[-1].start()

    def target_chip(way, k):
        return here.chip(far - k if way == 0 else k - far)

    def unit(way, k, h, src):
        sl = pl.ds(h * half, half)
        s = way * 8 + k * 2 + h
        return pltpu.make_async_remote_copy(
            src_ref=src.at[sl, :], dst_ref=chain.at[way * far + k, sl, :], send_sem=chain_send.at[s], recv_sem=chain_recv.at[s],
            device_id=here.along[way], device_id_type=MESH)

    def forward(way, k, h):
        arrived = chain.at[way * far + k]
        unit(way, k, h, arrived).wait_recv()
        sl = pl.ds(h * half, half)
        arrived[sl, :] = (arrived[sl, :].astype(F32) + own[target_chip(way, k + 1), sl, :].astype(F32)).astype(BF16)
        unit(way, k + 1, h, arrived).start()

    loads[0].wait()
    for way in range(2):
        unit(way, 0, way, own.at[target_chip(way, 0)]).start()
    for way in range(2):
        unit(way, 1, 1 - way, own.at[target_chip(way, 1)]).start()

    weight = mask_ref[...]
    count = jnp.maximum(jnp.sum(weight, keepdims=True)[0], 1.0)
    second = [
        pltpu.make_async_remote_copy(
            src_ref=every.at[me], dst_ref=every.at[me], send_sem=send2.at[d], recv_sem=recv2.at[d],
            device_id={'stage': peers[d]}, device_id_type=MESH)
        for d in range(1, n)
    ]

    def reduce_stats():
        for copy in first:
            copy.wait()
        parts = [st_ref[me]] + [got[d] for d in range(1, n)]
        m = functools.reduce(jnp.maximum, [p[0:1] for p in parts])
        total = sum(p[1:2] * jnp.exp(p[0:1] - m) for p in parts)
        target = sum(p[2:3] for p in parts)
        w = mask_ref[me]
        scale = w / count
        term = w * (jnp.log(total) + m - target)
        every[me] = jnp.concatenate([m, scale / total, scale, term, jnp.zeros((4, m.shape[1]), F32)], axis=0)

    loads[1].wait()
    loads[2].wait()
    tiles = y_hbm.shape[1] // MLP_TILE

    def piece(q, carry):
        m, i = q // layers, lax.rem(q, layers)
        slot = lax.rem(m, 2)

        @pl.when(i == 0)
        def _():
            @pl.when(m < tiles - 1)
            def _():
                load_a(m + 1).start()

            load_a(m).wait()

            @pl.when(m >= 2)
            def _():
                store_y(m - 2).wait()

            y_buf[slot] = a_buf[slot]

        @pl.when(is_middle())
        def _():
            y_buf[slot] = mlp_layer(y_buf[slot], upt_buf.at[i], down_buf.at[i])

        @pl.when(i == layers - 1)
        def _():
            store_y(m).start()

        @pl.when(q == 1)
        def _():
            for way in range(2):
                forward(way, 0, way)
            reduce_stats()
            for copy in second:
                copy.start()

        for at, (k, flip) in {2: (1, 1), 3: (1, 0), 4: (2, 1), 6: (2, 0)}.items():
            @pl.when(q == at)
            def _():
                for way in range(2):
                    forward(way, k, 1 - way if flip else way)
        return carry

    lax.fori_loop(0, tiles * layers, piece, 0)
    for copy in second:
        copy.wait()
    out_ref[...] = every[...]
    loss_ref[...] = jnp.broadcast_to(jnp.sum(every[:, 3, :], keepdims=True) / count, loss_ref.shape)
    for h in range(2):
        for way in range(2):
            unit(way, far - 1, h, own.at[0]).wait_recv()
    total = own[here.z].astype(F32) + (chain[far - 1].astype(F32) + chain[2 * far - 1].astype(F32))
    h_ref[...] = total.astype(BF16)
    for way in range(2):
        for k in range(far):
            for h in range(2):
                if k > 0 or h == way:
                    unit(way, k, h, own.at[0]).wait_send()
    for m in range(tiles - 2, tiles):
        store_y(m).wait()


def stats(st, mask, hsum, at, upt, down):
    n, _, tok = st.shape
    chips, dim, _ = hsum.shape
    tokens = MLP_STATS * MLP_TILE
    vmem = pl.BlockSpec(memory_space=pltpu.VMEM)
    anywhere = pl.BlockSpec(memory_space=pl.ANY)
    dma = pltpu.SemaphoreType.DMA
    return pl.pallas_call(
        functools.partial(stats_kernel, n),
        in_specs=[vmem, vmem] + [anywhere] * 4,
        out_specs=[vmem, vmem, vmem, anywhere],
        out_shape=[
            jax.ShapeDtypeStruct((n, 8, tok), F32),
            jax.ShapeDtypeStruct((8, 128), F32),
            jax.ShapeDtypeStruct((dim, tok), BF16),
            jax.ShapeDtypeStruct((dim, tokens), BF16),
        ],
        scratch_shapes=[
            pltpu.VMEM((n, 8, tok), F32),
            pltpu.VMEM((n, 8, tok), F32),
            pltpu.VMEM((chips, dim, tok), BF16),
            pltpu.VMEM((chips, dim, tok), BF16),
            pltpu.VMEM(upt.shape, BF16),
            pltpu.VMEM(down.shape, BF16),
            pltpu.VMEM((2, dim, MLP_TILE), BF16),
            pltpu.VMEM((2, dim, MLP_TILE), BF16),
            dma((n,)), dma((n,)), dma((n,)), dma((n,)), dma((3,)), dma((16,)), dma((16,)), dma((2,)), dma((2,)),
        ],
        compiler_params=params(56, collective_id=0, has_side_effects=True),
        cost_estimate=cost(3e10, 2e7),
        name='stats',
    )(st, mask, hsum, at, upt, down)


def grad_kernel(n, e_hbm, w_hbm, x_hbm, a_hbm, upt_hbm, down_hbm, cm_ref, gs_ref, lab_ref, dx_ref, dw_hbm, y_hbm, g_buf, send_buf,
                own, pair, chain, load_sem, e_sem, pair_send, pair_recv, chain_send, chain_recv, a_sem, y_sem):
    stage = lax.axis_index('stage')
    chips = n // 2
    far = chips // 2
    z, core = stage // 2, lax.rem(stage, 2)
    dim, tok = dx_ref.shape
    rows = w_hbm.shape[1]
    half = dim // 2
    partner = {'stage': 2 * z + 1 - core}
    ahead = {'stage': 2 * lax.rem(z + 1, chips) + core}
    behind = {'stage': 2 * lax.rem(z + chips - 1, chips) + core}

    def chip_at(i):
        size = far - (i + 1) // 2
        sign = 2 * lax.rem(i, 2) - 1
        return lax.rem(z + sign * size + chips, chips)

    def block_at(i, own_side):
        return 2 * chip_at(i) + (core if own_side else 1 - core)

    barrier = pltpu.get_barrier_semaphore()
    for peer in (partner, ahead, behind):
        pl.semaphore_signal(barrier, inc=1, device_id=peer, device_id_type=MESH)
    pl.semaphore_wait(barrier, 3)

    def pair_copy(i):
        return pltpu.make_async_remote_copy(
            src_ref=send_buf.at[lax.rem(i, 2)], dst_ref=pair.at[i], send_sem=pair_send.at[lax.rem(i, 2)],
            recv_sem=pair_recv.at[i], device_id=partner, device_id_type=MESH)

    def pair_add(i):
        pair_copy(i).wait_recv()
        own[i] += pair[i]

    def unit(way, k, h, src):
        sl = pl.ds(h * half, half)
        s = way * 8 + k * 2 + h
        return pltpu.make_async_remote_copy(
            src_ref=src.at[sl, :], dst_ref=chain.at[way * far + k, sl, :], send_sem=chain_send.at[s], recv_sem=chain_recv.at[s],
            device_id=ahead if way == 0 else behind, device_id_type=MESH)

    def place(way, k):
        return 0 if k == 0 else 2 * k - 1 + way

    def first_send(way):
        unit(way, 0, way, own.at[0]).start()

    def plain_send(way):
        unit(way, 1, 1 - way, own.at[place(way, 1)]).start()

    def forward(way, k, h):
        here = chain.at[way * far + k]
        unit(way, k, h, here).wait_recv()
        sl = pl.ds(h * half, half)
        here[sl, :] += own[place(way, k + 1), sl, :]
        unit(way, k + 1, h, here).start()

    def gradients(w_buf, e_buf):
        def load_e(i, q):
            slot = lax.rem(i, 2)
            return pltpu.make_async_copy(e_hbm.at[block_at(i, q == 1)], e_buf.at[slot, q], e_sem.at[slot, q])

        for q in range(2):
            load_e(0, q).start()
        load_w = pltpu.make_async_copy(w_hbm, w_buf, load_sem.at[0])
        load_w.start()
        index = lax.broadcasted_iota(jnp.int32, (CHUNK, tok), 0)
        load_w.wait()

        def body(i, carry):
            @pl.when(i < chips - 1)
            def _():
                for q in range(2):
                    load_e(i + 1, q).start()

            @pl.when(i >= 2)
            def _():
                pair_copy(i - 2).wait_send()

            for q in range(2):
                load_e(i, q).wait()
            slot = lax.rem(i, 2)
            blocks = [block_at(i, q == 1) for q in range(2)]
            parts = [[], []]
            for q in range(2):
                gs, cm, lab = gs_ref[blocks[q]], cm_ref[blocks[q]], lab_ref[blocks[q]]
                m, over, scale = gs[0:1], gs[1:2], gs[2:3]
                for c in range(rows // CHUNK):
                    sl = pl.ds(c * CHUNK, CHUNK)
                    p = e_buf[slot, q, sl, :] * (jnp.exp(cm[c:c + 1] - m) * over)
                    g = jnp.where(index == lab - c * CHUNK, p - scale, p).astype(BF16)
                    g_buf[blocks[q], sl, :] = g
                    parts[q].append(g)
            both = jnp.concatenate([jnp.concatenate(p, axis=0) for p in parts], axis=1)
            dx = mm(w_buf[...], both, 1, 0)
            send_buf[slot] = dx[:, :tok]
            own[i] = dx[:, tok:]
            pair_copy(i).start()

            @pl.when(i >= 1)
            def _():
                pair_add(i - 1)

            @pl.when(i == 1)
            def _():
                first_send(0)
                first_send(1)

            @pl.when(i == 2)
            def _():
                plain_send(0)

            @pl.when(i == 3)
            def _():
                plain_send(1)

            @pl.when(i == chips - 2)
            def _():
                for way in range(2):
                    forward(way, 0, way)
            return carry

        lax.fori_loop(0, chips, body, 0)

    pl.run_scoped(gradients, pltpu.VMEM((dim, rows), BF16), pltpu.VMEM((2, 2, rows, tok), F32))
    pair_add(chips - 1)

    def fill(x_buf, upt_buf, down_buf, a_buf, y_buf, dw_buf):
        loads = [
            pltpu.make_async_copy(src, dst, load_sem.at[k])
            for k, (src, dst) in enumerate([(x_hbm, x_buf), (upt_hbm, upt_buf), (down_hbm, down_buf)])
        ]
        for load in loads:
            load.start()
        tiles = y_hbm.shape[1] // MLP_TILE

        def cols(m):
            return pl.ds(pl.multiple_of(m * MLP_TILE, MLP_TILE), MLP_TILE)

        def load_a(m):
            slot = lax.rem(m, 2)
            return pltpu.make_async_copy(a_hbm.at[:, cols(m + MLP_GATHER + MLP_STATS)], a_buf.at[slot], a_sem.at[slot])

        def store_y(m):
            slot = lax.rem(m, 2)
            return pltpu.make_async_copy(y_buf.at[slot], y_hbm.at[:, cols(m)], y_sem.at[slot])

        load_a(0).start()
        loads[0].wait()
        width = 512
        pieces = rows // width

        def store_dw(j):
            slot = lax.rem(j, 2)
            start = pl.multiple_of(j * width, width)
            return pltpu.make_async_copy(dw_buf.at[slot], dw_hbm.at[:, pl.ds(start, width)], y_sem.at[slot])

        def head(j, carry):
            start = pl.multiple_of(j * width, width)
            g = jnp.concatenate([g_buf[b, pl.ds(start, width), :] for b in range(n)], axis=1)

            @pl.when(j >= 2)
            def _():
                store_dw(j - 2).wait()

            dw_buf[lax.rem(j, 2)] = mm(side_by_side(x_buf), g, 1, 1).astype(BF16)
            store_dw(j).start()

            @pl.when(j == 0)
            def _():
                for way in range(2):
                    forward(way, 1, 1 - way)

            @pl.when(j == 2)
            def _():
                for way in range(2):
                    forward(way, 1, way)

            @pl.when(j == 4)
            def _():
                for way in range(2):
                    forward(way, 2, 1 - way)
            return carry

        lax.fori_loop(0, pieces, head, 0)
        for j in range(pieces - 2, pieces):
            store_dw(j).wait()
        loads[1].wait()
        loads[2].wait()

        def layers(m, carry):
            slot = lax.rem(m, 2)

            @pl.when(m < tiles - 1)
            def _():
                load_a(m + 1).start()

            load_a(m).wait()

            @pl.when(m >= 2)
            def _():
                store_y(m - 2).wait()

            @pl.when(is_middle())
            def _():
                h = a_buf[slot]
                for i in range(upt_buf.shape[0]):
                    h = mlp_layer(h, upt_buf.at[i], down_buf.at[i])
                y_buf[slot] = h

            @pl.when(jnp.logical_not(is_middle()))
            def _():
                y_buf[slot] = a_buf[slot]

            store_y(m).start()

            @pl.when(m == 0)
            def _():
                for way in range(2):
                    forward(way, 2, way)
            return carry

        lax.fori_loop(0, tiles, layers, 0)
        for m in range(tiles - 2, tiles):
            store_y(m).wait()

    pl.run_scoped(
        fill, pltpu.VMEM(x_hbm.shape, BF16), pltpu.VMEM(upt_hbm.shape, BF16), pltpu.VMEM(down_hbm.shape, BF16),
        pltpu.VMEM((2, dim, MLP_TILE), BF16), pltpu.VMEM((2, dim, MLP_TILE), BF16), pltpu.VMEM((2, dim, 512), BF16))
    for h in range(2):
        for way in range(2):
            unit(way, far - 1, h, own.at[0]).wait_recv()
    dx_ref[...] = own[chips - 1] + (chain[far - 1] + chain[2 * far - 1])
    for i in range(chips - 2, chips):
        pair_copy(i).wait_send()
    for way in range(2):
        for k in range(far):
            for h in range(2):
                if k > 0 or h == way:
                    unit(way, k, h, own.at[0]).wait_send()


def grad(wt, e, x, at, upt, down, cm, gs, lab):
    dim, rows = wt.shape
    n, _, tok = e.shape
    chips = n // 2
    tokens = at.shape[1] - (MLP_GATHER + MLP_STATS) * MLP_TILE
    vmem = pl.BlockSpec(memory_space=pltpu.VMEM)
    anywhere = pl.BlockSpec(memory_space=pl.ANY)
    dma = pltpu.SemaphoreType.DMA
    return pl.pallas_call(
        functools.partial(grad_kernel, n),
        in_specs=[anywhere] * 6 + [vmem] * 3,
        out_specs=[vmem, anywhere, anywhere],
        out_shape=[
            jax.ShapeDtypeStruct((dim, tok), F32),
            jax.ShapeDtypeStruct((dim, rows), BF16),
            jax.ShapeDtypeStruct((dim, tokens), BF16),
        ],
        scratch_shapes=[
            pltpu.VMEM((n, rows, tok), BF16),
            pltpu.VMEM((2, dim, tok), F32),
            pltpu.VMEM((chips, dim, tok), F32),
            pltpu.VMEM((chips, dim, tok), F32),
            pltpu.VMEM((chips, dim, tok), F32),
            dma((3,)), dma((2, 2)), dma((2,)), dma((chips,)), dma((16,)), dma((16,)), dma((2,)), dma((2,)),
        ],
        compiler_params=pltpu.CompilerParams(vmem_limit_bytes=63 * MIB, collective_id=1, has_side_effects=True),
        cost_estimate=cost(6 * n * tok * dim * rows, 6 * n * tok * rows),
        name='grad',
    )(e, wt, x, at, upt, down, cm, gs, lab)


def solution(mesh):
    n = mesh.shape['stage']
    row_spec = P(('data', 'stage'), None)
    vocab_spec = P('stage', None)
    layer_spec = P('stage', None, None, None)
    acts_spec = P(('data', 'stage'), None, None)

    def per_device(x_loc, w_loc, labels, loss_mask, e_loc, next_ids, acts_loc, up_loc, down_loc):
        tok = x_loc.shape[0]
        offset = lax.axis_index('stage') * w_loc.shape[0]
        wt, at, down = w_loc.T, acts_loc[0].T, jnp.swapaxes(down_loc[0], 1, 2)
        ids = (next_ids - offset).reshape(n, 1, tok)
        lab = (labels - offset).reshape(n, 1, tok)
        mask = loss_mask.astype(F32).reshape(n, 1, tok)
        x, hsum, y0, upt = gather(x_loc.T, ids, e_loc.T, up_loc[0], down, at)
        e, cm, st = logits(wt, x, lab)
        gs, loss, embed_rows, y1 = stats(st, mask, hsum, at, upt, down)
        dx, dw, y2 = grad(wt, e, x, at, upt, down, cm, gs, lab)
        stage_out = jnp.concatenate([y0, y1, y2], axis=1)
        return loss[0, :1], dx.T, dw.T, embed_rows.T, stage_out.T[None]

    return jax.shard_map(
        per_device,
        mesh=mesh,
        in_specs=(row_spec, vocab_spec, P('data'), P('data'), vocab_spec, P('data'), acts_spec, layer_spec, layer_spec),
        out_specs=(P('data'), row_spec, row_spec, row_spec, acts_spec),
        check_vma=False,
    )
```

```python
import functools

import jax
import jax.numpy as jnp
from jax import lax
from jax.experimental import pallas as pl
from jax.experimental.pallas import tpu as pltpu
from jax.sharding import PartitionSpec as P

F32 = jnp.float32
BF16 = jnp.bfloat16
MESH = pl.DeviceIdType.MESH
CHUNK = 512
GROUP = 2
MIB = 1024 * 1024


def mm(a, b, ca, cb):
    return lax.dot_general(a, b, (((ca,), (cb,)), ((), ())), preferred_element_type=F32)


def params(limit, **kw):
    return pltpu.CompilerParams(vmem_limit_bytes=limit * MIB, **kw)


def cost(flops, nbytes):
    return pl.CostEstimate(flops=int(flops), bytes_accessed=int(nbytes), transcendentals=0)


def transpose_into(dst_ref, src, step):
    for c in range(0, src.shape[1], step):
        dst_ref[pl.ds(c, step), :] = src[:, c:c + step].T


def side_by_side(ref):
    return jnp.concatenate([ref[b] for b in range(ref.shape[0])], axis=1)


def gelu(x):
    k = 0.7978845608028654
    inner = x * (k + (k * 0.044715) * (x * x))
    half = 0.5 * x
    return half + half * jnp.tanh(inner)


MLP_TILE = 512
MLP_GATHER = 2
MLP_STATS = 3


def mlp_layer(h, upt, down):
    hidden = upt.shape[0]
    u = jnp.concatenate(
        [gelu(mm(upt[pl.ds(c, 512), :], h, 1, 0)).astype(BF16) for c in range(0, hidden, 512)], axis=0)
    return (h.astype(F32) + mm(down[...], u, 1, 0)).astype(BF16)


def is_middle():
    stage = lax.axis_index('stage')
    return (stage > 0) & (stage < lax.axis_size('stage') - 1)


class Place:
    def __init__(self, n):
        stage = lax.axis_index('stage')
        self.chips = n // 2
        self.far = self.chips // 2
        self.z, self.core = stage // 2, lax.rem(stage, 2)
        self.partner = {'stage': 2 * self.z + 1 - self.core}
        self.along = [{'stage': 2 * self.chip(1) + self.core}, {'stage': 2 * self.chip(-1) + self.core}]

    def chip(self, steps):
        return lax.rem(self.z + steps + self.chips, self.chips)

    def block(self, chip, own_side):
        return 2 * chip + (self.core if own_side else 1 - self.core)

    def greet(self, barrier):
        for peer in [self.partner] + self.along:
            pl.semaphore_signal(barrier, inc=1, device_id=peer, device_id_type=MESH)
        pl.semaphore_wait(barrier, 3)


def gather_kernel(n, x_ref, ids_ref, et_hbm, up_hbm, down_hbm, a_hbm, x_out, h_out, y_out, upt_out, x_all, et, up_buf, upt_buf,
                  down_buf, a_buf, y_buf, send_buf, own, pair, load_sem, out_sem, ring_send, ring_recv, side_send, side_recv,
                  pair_send, pair_recv):
    here = Place(n)
    dim, tok = x_ref.shape
    half = dim // 2
    rows = et.shape[1]
    layers = up_buf.shape[0]
    mine = here.block(here.z, True)
    loads = [
        pltpu.make_async_copy(src, dst, load_sem.at[k])
        for k, (src, dst) in enumerate([
            (et_hbm, et), (up_hbm, up_buf), (down_hbm, down_buf), (a_hbm.at[:, pl.ds(0, MLP_GATHER * MLP_TILE)], a_buf), (x_ref, x_all.at[mine])])
    ]
    for load in loads:
        load.start()
    here.greet(pltpu.get_barrier_semaphore())

    def unit(way, k, h):
        sl = pl.ds(h * half, half)
        block = here.block(here.chip(k if way else -k), True)
        src = x_ref.at[sl, :] if k == 0 else x_all.at[block, sl, :]
        s = way * 8 + k * 2 + h
        return pltpu.make_async_remote_copy(
            src_ref=src, dst_ref=x_all.at[block, sl, :], send_sem=ring_send.at[s], recv_sem=ring_recv.at[s],
            device_id=here.along[way], device_id_type=MESH)

    def side(way, k, h):
        sl = pl.ds(h * half, half)
        block = here.block(here.chip(1 + k if way else -1 - k), True)
        s = way * 8 + k * 2 + h
        return pltpu.make_async_remote_copy(
            src_ref=x_all.at[block, sl, :], dst_ref=x_all.at[block, sl, :], send_sem=side_send.at[s], recv_sem=side_recv.at[s],
            device_id=here.partner, device_id_type=MESH)

    def side_mine():
        return pltpu.make_async_remote_copy(
            src_ref=x_ref, dst_ref=x_all.at[mine], send_sem=side_send.at[16], recv_sem=side_recv.at[16],
            device_id=here.partner, device_id_type=MESH)

    last = here.far - 1
    arrivals = [[(k, h) for k in range(last) for h in range(2)] + [(last, way)] for way in range(2)]

    def event(u):
        for way in range(2):
            k, h = arrivals[way][u]
            unit(way, k, h).wait_recv()
            if (k + 1, h) in arrivals[way]:
                unit(way, k + 1, h).start()
            side(way, k, h).start()

    for h in range(2):
        for way in range(2):
            unit(way, 0, h).start()
    side_mine().start()

    def pair_copy(i):
        return pltpu.make_async_remote_copy(
            src_ref=send_buf.at[lax.rem(i, 2)], dst_ref=pair.at[i], send_sem=pair_send.at[lax.rem(i, 2)],
            recv_sem=pair_recv.at[i], device_id=here.partner, device_id_type=MESH)

    def pair_add(i):
        pair_copy(i).wait_recv()
        own[i] = (own[i].astype(F32) + pair[i].astype(F32)).astype(BF16)

    loads[0].wait()
    index = lax.broadcasted_iota(jnp.int32, (rows, 2 * tok), 0)

    def embed(i, carry):
        @pl.when(i >= 2)
        def _():
            pair_copy(i - 2).wait_send()

        ids = jnp.concatenate([ids_ref[here.block(i, False)], ids_ref[here.block(i, True)]], axis=1)
        hot = jnp.where(index == ids, 1.0, 0.0).astype(BF16)
        out = mm(et[...], hot, 1, 0).astype(BF16)
        send_buf[lax.rem(i, 2)] = out[:, :tok]
        own[i] = out[:, tok:]
        pair_copy(i).start()

        @pl.when(i >= 1)
        def _():
            pair_add(i - 1)

        for u in range(here.chips - 2):
            @pl.when(i == u + 2)
            def _():
                event(u)
        return carry

    lax.fori_loop(0, here.chips, embed, 0)
    loads[1].wait()
    for i in range(layers):
        transpose_into(upt_buf.at[i], up_buf[i], 256)
    loads[2].wait()
    loads[3].wait()
    def tiles(m, carry):
        cols = pl.ds(pl.multiple_of(m * MLP_TILE, MLP_TILE), MLP_TILE)

        @pl.when(is_middle())
        def _():
            h = a_buf[:, cols]
            for i in range(layers):
                h = mlp_layer(h, upt_buf.at[i], down_buf.at[i])
            y_buf[:, cols] = h

        @pl.when(jnp.logical_not(is_middle()))
        def _():
            y_buf[:, cols] = a_buf[:, cols]
        return carry

    lax.fori_loop(0, 1, tiles, 0)
    event(here.chips - 2)
    pair_add(here.chips - 1)
    outs = [
        pltpu.make_async_copy(src, dst, out_sem.at[k])
        for k, (src, dst) in enumerate([(own, h_out), (upt_buf, upt_out), (x_all, x_out), (y_buf, y_out)])
    ]
    outs[0].start()
    outs[1].start()
    loads[4].wait()
    side_mine().wait()
    for way in range(2):
        for k, h in arrivals[way]:
            side(way, k, h).wait()
    outs[2].start()
    lax.fori_loop(1, MLP_GATHER, tiles, 0)
    outs[3].start()
    for way in range(2):
        for k, h in arrivals[way]:
            unit(way, k, h).wait_send()
    for i in range(here.chips - 2, here.chips):
        pair_copy(i).wait_send()
    for out in outs:
        out.wait()


def gather(xt, ids, et, up, down, at):
    dim, tok = xt.shape
    n = ids.shape[0]
    rows = et.shape[1]
    layers, _, hidden = up.shape
    tokens = MLP_GATHER * MLP_TILE
    vmem = pl.BlockSpec(memory_space=pltpu.VMEM)
    anywhere = pl.BlockSpec(memory_space=pl.ANY)
    dma = pltpu.SemaphoreType.DMA
    return pl.pallas_call(
        functools.partial(gather_kernel, n),
        in_specs=[vmem, vmem] + [anywhere] * 4,
        out_specs=[anywhere] * 4,
        out_shape=[
            jax.ShapeDtypeStruct((n, dim, tok), BF16),
            jax.ShapeDtypeStruct((n // 2, dim, tok), BF16),
            jax.ShapeDtypeStruct((dim, tokens), BF16),
            jax.ShapeDtypeStruct((layers, hidden, dim), BF16),
        ],
        scratch_shapes=[
            pltpu.VMEM((n, dim, tok), BF16),
            pltpu.VMEM((dim, rows), BF16),
            pltpu.VMEM((layers, dim, hidden), BF16),
            pltpu.VMEM((layers, hidden, dim), BF16),
            pltpu.VMEM((layers, dim, hidden), BF16),
            pltpu.VMEM((dim, tokens), BF16),
            pltpu.VMEM((dim, tokens), BF16),
            pltpu.VMEM((2, dim, tok), BF16),
            pltpu.VMEM((n // 2, dim, tok), BF16),
            pltpu.VMEM((n // 2, dim, tok), BF16),
            dma((5,)), dma((4,)), dma((16,)), dma((16,)), dma((17,)), dma((17,)), dma((2,)), dma((n // 2,)),
        ],
        compiler_params=params(56, collective_id=2, has_side_effects=True),
        cost_estimate=cost(2 * n * tok * dim * rows, 4 * n * tok * dim),
        name='gather',
    )(xt, ids, et, up, down, at)


def logits_kernel(n, wt_ref, x_ref, lab_ref, h_hbm, e_ref, cm_ref, st_ref, h_ref, w_ref, own, chain, load_sem, chain_send, chain_recv):
    here = Place(n)
    far = here.far
    half = h_ref.shape[0] // 2
    step = pl.program_id(0)
    load = pltpu.make_async_copy(h_hbm, own, load_sem.at[0])

    @pl.when(step == 0)
    def _():
        load.start()
        here.greet(pltpu.get_barrier_semaphore())

    def target_chip(way, k):
        return here.chip(far - k if way == 0 else k - far)

    def unit(way, k, h, src):
        sl = pl.ds(h * half, half)
        s = way * 8 + k * 2 + h
        return pltpu.make_async_remote_copy(
            src_ref=src.at[sl, :], dst_ref=chain.at[way * far + k, sl, :], send_sem=chain_send.at[s], recv_sem=chain_recv.at[s],
            device_id=here.along[way], device_id_type=MESH)

    def forward(way, k, h):
        arrived = chain.at[way * far + k]
        unit(way, k, h, arrived).wait_recv()
        sl = pl.ds(h * half, half)
        arrived[sl, :] = (arrived[sl, :].astype(F32) + own[target_chip(way, k + 1), sl, :].astype(F32)).astype(BF16)
        unit(way, k + 1, h, arrived).start()

    rows = wt_ref.shape[1]
    tok = x_ref.shape[2]

    @pl.when(pl.program_id(0) == 0)
    def _():
        transpose_into(w_ref, wt_ref, 256)

    x = side_by_side(x_ref)
    lab = side_by_side(lab_ref)
    index = lax.broadcasted_iota(jnp.int32, (CHUNK, GROUP * tok), 0)
    maxes, sums = [], []
    target = jnp.zeros((1, GROUP * tok), F32)
    for c in range(rows // CHUNK):
        sl = pl.ds(c * CHUNK, CHUNK)
        z = mm(w_ref[sl, :], x, 1, 0)
        m = jnp.max(z, axis=0, keepdims=True)
        e = jnp.exp(z - m)
        for b in range(GROUP):
            e_ref[b, sl, :] = e[:, b * tok:(b + 1) * tok]
        maxes.append(m)
        sums.append(jnp.sum(e, axis=0, keepdims=True))
        target += jnp.sum(jnp.where(index == lab - c * CHUNK, z, 0.0), axis=0, keepdims=True)
    m = functools.reduce(jnp.maximum, maxes)
    s = sum(si * jnp.exp(mi - m) for mi, si in zip(maxes, sums))
    cm = jnp.concatenate(maxes + [jnp.zeros((8 - len(maxes), GROUP * tok), F32)], axis=0)
    st = jnp.concatenate([m, s, target, jnp.zeros((5, GROUP * tok), F32)], axis=0)
    for b in range(GROUP):
        cm_ref[b] = cm[:, b * tok:(b + 1) * tok]
        st_ref[b] = st[:, b * tok:(b + 1) * tok]

    @pl.when(step == 0)
    def _():
        load.wait()
        for way in range(2):
            unit(way, 0, way, own.at[target_chip(way, 0)]).start()
        for way in range(2):
            unit(way, 1, 1 - way, own.at[target_chip(way, 1)]).start()

    @pl.when(step == 2)
    def _():
        for way in range(2):
            forward(way, 0, way)
        for way in range(2):
            forward(way, 1, 1 - way)

    @pl.when(step == 4)
    def _():
        for way in range(2):
            forward(way, 1, way)
        for way in range(2):
            forward(way, 2, 1 - way)

    @pl.when(step == 6)
    def _():
        for way in range(2):
            forward(way, 2, way)

    @pl.when(step == 7)
    def _():
        for h in range(2):
            for way in range(2):
                unit(way, far - 1, h, own.at[0]).wait_recv()
        total = own[here.z].astype(F32) + (chain[far - 1].astype(F32) + chain[2 * far - 1].astype(F32))
        h_ref[...] = total.astype(BF16)
        for way in range(2):
            for k in range(far):
                for h in range(2):
                    if k > 0 or h == way:
                        unit(way, k, h, own.at[0]).wait_send()


def logits(wt, x, lab, hsum):
    dim, rows = wt.shape
    n, _, tok = x.shape
    block = lambda r, c: pl.BlockSpec((GROUP, r, c), lambda i: (i, 0, 0))
    dma = pltpu.SemaphoreType.DMA
    return pl.pallas_call(
        functools.partial(logits_kernel, n),
        grid=(n // GROUP,),
        in_specs=[
            pl.BlockSpec((dim, rows), lambda i: (0, 0)), block(dim, tok), block(1, tok), pl.BlockSpec(memory_space=pl.ANY)],
        out_specs=[block(rows, tok), block(8, tok), block(8, tok), pl.BlockSpec((dim, tok), lambda i: (0, 0))],
        out_shape=[
            jax.ShapeDtypeStruct((n, rows, tok), F32),
            jax.ShapeDtypeStruct((n, 8, tok), F32),
            jax.ShapeDtypeStruct((n, 8, tok), F32),
            jax.ShapeDtypeStruct((dim, tok), BF16),
        ],
        scratch_shapes=[
            pltpu.VMEM((rows, dim), BF16), pltpu.VMEM(hsum.shape, BF16), pltpu.VMEM(hsum.shape, BF16),
            dma((1,)), dma((16,)), dma((16,)),
        ],
        compiler_params=params(56, collective_id=3, has_side_effects=True),
        cost_estimate=cost(2 * n * tok * dim * rows, 4 * n * tok * rows),
        name='logits',
    )(wt, x, lab, hsum)


def stats_kernel(n, st_ref, mask_ref, a_hbm, upt_hbm, down_hbm, out_ref, loss_ref, y_hbm, got, every, upt_buf, down_buf, a_buf,
                 y_buf, send1, recv1, send2, recv2, load_sem, a_sem, y_sem):
    me = lax.axis_index('stage')
    layers = upt_buf.shape[0]
    loads = [
        pltpu.make_async_copy(src, dst, load_sem.at[k])
        for k, (src, dst) in enumerate([(upt_hbm, upt_buf), (down_hbm, down_buf)])
    ]
    for load in loads:
        load.start()

    def load_a(m):
        start = pl.multiple_of((m + MLP_GATHER) * MLP_TILE, MLP_TILE)
        slot = lax.rem(m, 2)
        return pltpu.make_async_copy(a_hbm.at[:, pl.ds(start, MLP_TILE)], a_buf.at[slot], a_sem.at[slot])

    def store_y(m):
        slot = lax.rem(m, 2)
        start = pl.multiple_of(m * MLP_TILE, MLP_TILE)
        return pltpu.make_async_copy(y_buf.at[slot], y_hbm.at[:, pl.ds(start, MLP_TILE)], y_sem.at[slot])

    load_a(0).start()
    barrier = pltpu.get_barrier_semaphore()
    peers = [lax.rem(me + d, n) for d in range(n)]
    for d in range(1, n):
        pl.semaphore_signal(barrier, inc=1, device_id={'stage': peers[d]}, device_id_type=MESH)
    pl.semaphore_wait(barrier, n - 1)

    first = []
    for d in range(1, n):
        first.append(pltpu.make_async_remote_copy(
            src_ref=st_ref.at[peers[d]], dst_ref=got.at[d], send_sem=send1.at[d], recv_sem=recv1.at[d],
            device_id={'stage': peers[d]}, device_id_type=MESH))
        first[-1].start()

    weight = mask_ref[...]
    count = jnp.maximum(jnp.sum(weight, keepdims=True)[0], 1.0)
    second = [
        pltpu.make_async_remote_copy(
            src_ref=every.at[me], dst_ref=every.at[me], send_sem=send2.at[d], recv_sem=recv2.at[d],
            device_id={'stage': peers[d]}, device_id_type=MESH)
        for d in range(1, n)
    ]

    def reduce_stats():
        for copy in first:
            copy.wait()
        parts = [st_ref[me]] + [got[d] for d in range(1, n)]
        m = functools.reduce(jnp.maximum, [p[0:1] for p in parts])
        total = sum(p[1:2] * jnp.exp(p[0:1] - m) for p in parts)
        target = sum(p[2:3] for p in parts)
        w = mask_ref[me]
        scale = w / count
        term = w * (jnp.log(total) + m - target)
        every[me] = jnp.concatenate([m, scale / total, scale, term, jnp.zeros((4, m.shape[1]), F32)], axis=0)

    for load in loads:
        load.wait()
    tiles = y_hbm.shape[1] // MLP_TILE

    def piece(q, carry):
        m, i = q // layers, lax.rem(q, layers)
        slot = lax.rem(m, 2)

        @pl.when(i == 0)
        def _():
            @pl.when(m < tiles - 1)
            def _():
                load_a(m + 1).start()

            load_a(m).wait()

            @pl.when(m >= 2)
            def _():
                store_y(m - 2).wait()

            y_buf[slot] = a_buf[slot]

        @pl.when(is_middle())
        def _():
            y_buf[slot] = mlp_layer(y_buf[slot], upt_buf.at[i], down_buf.at[i])

        @pl.when(i == layers - 1)
        def _():
            store_y(m).start()

        @pl.when(q == 1)
        def _():
            reduce_stats()
            for copy in second:
                copy.start()

        return carry

    lax.fori_loop(0, tiles * layers, piece, 0)
    for copy in second:
        copy.wait()
    out_ref[...] = every[...]
    loss_ref[...] = jnp.broadcast_to(jnp.sum(every[:, 3, :], keepdims=True) / count, loss_ref.shape)
    for m in range(tiles - 2, tiles):
        store_y(m).wait()


def stats(st, mask, at, upt, down):
    n, _, tok = st.shape
    dim = at.shape[0]
    tokens = MLP_STATS * MLP_TILE
    vmem = pl.BlockSpec(memory_space=pltpu.VMEM)
    anywhere = pl.BlockSpec(memory_space=pl.ANY)
    dma = pltpu.SemaphoreType.DMA
    return pl.pallas_call(
        functools.partial(stats_kernel, n),
        in_specs=[vmem, vmem] + [anywhere] * 3,
        out_specs=[vmem, vmem, anywhere],
        out_shape=[
            jax.ShapeDtypeStruct((n, 8, tok), F32),
            jax.ShapeDtypeStruct((8, 128), F32),
            jax.ShapeDtypeStruct((dim, tokens), BF16),
        ],
        scratch_shapes=[
            pltpu.VMEM((n, 8, tok), F32),
            pltpu.VMEM((n, 8, tok), F32),
            pltpu.VMEM(upt.shape, BF16),
            pltpu.VMEM(down.shape, BF16),
            pltpu.VMEM((2, dim, MLP_TILE), BF16),
            pltpu.VMEM((2, dim, MLP_TILE), BF16),
            dma((n,)), dma((n,)), dma((n,)), dma((n,)), dma((2,)), dma((2,)), dma((2,)),
        ],
        compiler_params=params(56, collective_id=0, has_side_effects=True),
        cost_estimate=cost(3e10, 2e7),
        name='stats',
    )(st, mask, at, upt, down)


def grad_kernel(n, e_hbm, w_hbm, x_hbm, a_hbm, upt_hbm, down_hbm, cm_ref, gs_ref, lab_ref, dx_ref, dw_hbm, y_hbm, g_buf, send_buf,
                own, pair, chain, load_sem, e_sem, pair_send, pair_recv, chain_send, chain_recv, a_sem, y_sem):
    stage = lax.axis_index('stage')
    chips = n // 2
    far = chips // 2
    z, core = stage // 2, lax.rem(stage, 2)
    dim, tok = dx_ref.shape
    rows = w_hbm.shape[1]
    half = dim // 2
    partner = {'stage': 2 * z + 1 - core}
    ahead = {'stage': 2 * lax.rem(z + 1, chips) + core}
    behind = {'stage': 2 * lax.rem(z + chips - 1, chips) + core}

    def chip_at(i):
        size = far - (i + 1) // 2
        sign = 2 * lax.rem(i, 2) - 1
        return lax.rem(z + sign * size + chips, chips)

    def block_at(i, own_side):
        return 2 * chip_at(i) + (core if own_side else 1 - core)

    def pair_copy(i):
        return pltpu.make_async_remote_copy(
            src_ref=send_buf.at[lax.rem(i, 2)], dst_ref=pair.at[i], send_sem=pair_send.at[lax.rem(i, 2)],
            recv_sem=pair_recv.at[i], device_id=partner, device_id_type=MESH)

    def pair_add(i):
        pair_copy(i).wait_recv()
        own[i] += pair[i]

    def unit(way, k, h, src):
        sl = pl.ds(h * half, half)
        s = way * 8 + k * 2 + h
        return pltpu.make_async_remote_copy(
            src_ref=src.at[sl, :], dst_ref=chain.at[way * far + k, sl, :], send_sem=chain_send.at[s], recv_sem=chain_recv.at[s],
            device_id=ahead if way == 0 else behind, device_id_type=MESH)

    def place(way, k):
        return 0 if k == 0 else 2 * k - 1 + way

    def first_send(way):
        unit(way, 0, way, own.at[0]).start()

    def plain_send(way):
        unit(way, 1, 1 - way, own.at[place(way, 1)]).start()

    def forward(way, k, h):
        here = chain.at[way * far + k]
        unit(way, k, h, here).wait_recv()
        sl = pl.ds(h * half, half)
        here[sl, :] += own[place(way, k + 1), sl, :]
        unit(way, k + 1, h, here).start()

    def gradients(w_buf, e_buf):
        def load_e(i, q):
            slot = lax.rem(i, 2)
            return pltpu.make_async_copy(e_hbm.at[block_at(i, q == 1)], e_buf.at[slot, q], e_sem.at[slot, q])

        for q in range(2):
            load_e(0, q).start()
        load_w = pltpu.make_async_copy(w_hbm, w_buf, load_sem.at[0])
        load_w.start()
        barrier = pltpu.get_barrier_semaphore()
        for peer in (partner, ahead, behind):
            pl.semaphore_signal(barrier, inc=1, device_id=peer, device_id_type=MESH)
        pl.semaphore_wait(barrier, 3)
        index = lax.broadcasted_iota(jnp.int32, (CHUNK, tok), 0)
        load_w.wait()

        def body(i, carry):
            @pl.when(i < chips - 1)
            def _():
                for q in range(2):
                    load_e(i + 1, q).start()

            @pl.when(i >= 2)
            def _():
                pair_copy(i - 2).wait_send()

            for q in range(2):
                load_e(i, q).wait()
            slot = lax.rem(i, 2)
            blocks = [block_at(i, q == 1) for q in range(2)]
            parts = [[], []]
            for q in range(2):
                gs, cm, lab = gs_ref[blocks[q]], cm_ref[blocks[q]], lab_ref[blocks[q]]
                m, over, scale = gs[0:1], gs[1:2], gs[2:3]
                for c in range(rows // CHUNK):
                    sl = pl.ds(c * CHUNK, CHUNK)
                    p = e_buf[slot, q, sl, :] * (jnp.exp(cm[c:c + 1] - m) * over)
                    g = jnp.where(index == lab - c * CHUNK, p - scale, p).astype(BF16)
                    g_buf[blocks[q], sl, :] = g
                    parts[q].append(g)
            both = jnp.concatenate([jnp.concatenate(p, axis=0) for p in parts], axis=1)
            dx = mm(w_buf[...], both, 1, 0)
            send_buf[slot] = dx[:, :tok]
            own[i] = dx[:, tok:]
            pair_copy(i).start()

            @pl.when(i >= 1)
            def _():
                pair_add(i - 1)

            @pl.when(i == 1)
            def _():
                first_send(0)
                first_send(1)

            @pl.when(i == 2)
            def _():
                plain_send(0)

            @pl.when(i == 3)
            def _():
                plain_send(1)

            @pl.when(i == chips - 2)
            def _():
                for way in range(2):
                    forward(way, 0, way)
            return carry

        lax.fori_loop(0, chips, body, 0)

    pl.run_scoped(gradients, pltpu.VMEM((dim, rows), BF16), pltpu.VMEM((2, 2, rows, tok), F32))
    pair_add(chips - 1)

    def fill(x_buf, upt_buf, down_buf, a_buf, y_buf, dw_buf):
        loads = [
            pltpu.make_async_copy(src, dst, load_sem.at[k])
            for k, (src, dst) in enumerate([(x_hbm, x_buf), (upt_hbm, upt_buf), (down_hbm, down_buf)])
        ]
        for load in loads:
            load.start()
        tiles = y_hbm.shape[1] // MLP_TILE

        def cols(m):
            return pl.ds(pl.multiple_of(m * MLP_TILE, MLP_TILE), MLP_TILE)

        def load_a(m):
            slot = lax.rem(m, 2)
            return pltpu.make_async_copy(a_hbm.at[:, cols(m + MLP_GATHER + MLP_STATS)], a_buf.at[slot], a_sem.at[slot])

        def store_y(m):
            slot = lax.rem(m, 2)
            return pltpu.make_async_copy(y_buf.at[slot], y_hbm.at[:, cols(m)], y_sem.at[slot])

        load_a(0).start()
        loads[0].wait()
        width = 512
        pieces = rows // width

        def store_dw(j):
            slot = lax.rem(j, 2)
            start = pl.multiple_of(j * width, width)
            return pltpu.make_async_copy(dw_buf.at[slot], dw_hbm.at[:, pl.ds(start, width)], y_sem.at[slot])

        def head(j, carry):
            start = pl.multiple_of(j * width, width)
            g = jnp.concatenate([g_buf[b, pl.ds(start, width), :] for b in range(n)], axis=1)

            @pl.when(j >= 2)
            def _():
                store_dw(j - 2).wait()

            dw_buf[lax.rem(j, 2)] = mm(side_by_side(x_buf), g, 1, 1).astype(BF16)
            store_dw(j).start()

            @pl.when(j == 0)
            def _():
                for way in range(2):
                    forward(way, 1, 1 - way)

            @pl.when(j == 2)
            def _():
                for way in range(2):
                    forward(way, 1, way)

            @pl.when(j == 4)
            def _():
                for way in range(2):
                    forward(way, 2, 1 - way)

            @pl.when(j == pieces - 1)
            def _():
                for way in range(2):
                    forward(way, 2, way)
            return carry

        lax.fori_loop(0, pieces, head, 0)
        for j in range(pieces - 2, pieces):
            store_dw(j).wait()
        loads[1].wait()
        loads[2].wait()

        def layers(m, carry):
            slot = lax.rem(m, 2)

            @pl.when(m < tiles - 1)
            def _():
                load_a(m + 1).start()

            load_a(m).wait()

            @pl.when(m >= 2)
            def _():
                store_y(m - 2).wait()

            @pl.when(is_middle())
            def _():
                h = a_buf[slot]
                for i in range(upt_buf.shape[0]):
                    h = mlp_layer(h, upt_buf.at[i], down_buf.at[i])
                y_buf[slot] = h

            @pl.when(jnp.logical_not(is_middle()))
            def _():
                y_buf[slot] = a_buf[slot]

            store_y(m).start()
            return carry

        lax.fori_loop(0, tiles, layers, 0)
        for m in range(tiles - 2, tiles):
            store_y(m).wait()

    pl.run_scoped(
        fill, pltpu.VMEM(x_hbm.shape, BF16), pltpu.VMEM(upt_hbm.shape, BF16), pltpu.VMEM(down_hbm.shape, BF16),
        pltpu.VMEM((2, dim, MLP_TILE), BF16), pltpu.VMEM((2, dim, MLP_TILE), BF16), pltpu.VMEM((2, dim, 512), BF16))
    for h in range(2):
        for way in range(2):
            unit(way, far - 1, h, own.at[0]).wait_recv()
    dx_ref[...] = own[chips - 1] + (chain[far - 1] + chain[2 * far - 1])
    for i in range(chips - 2, chips):
        pair_copy(i).wait_send()
    for way in range(2):
        for k in range(far):
            for h in range(2):
                if k > 0 or h == way:
                    unit(way, k, h, own.at[0]).wait_send()


def grad(wt, e, x, at, upt, down, cm, gs, lab):
    dim, rows = wt.shape
    n, _, tok = e.shape
    chips = n // 2
    tokens = at.shape[1] - (MLP_GATHER + MLP_STATS) * MLP_TILE
    vmem = pl.BlockSpec(memory_space=pltpu.VMEM)
    anywhere = pl.BlockSpec(memory_space=pl.ANY)
    dma = pltpu.SemaphoreType.DMA
    return pl.pallas_call(
        functools.partial(grad_kernel, n),
        in_specs=[anywhere] * 6 + [vmem] * 3,
        out_specs=[vmem, anywhere, anywhere],
        out_shape=[
            jax.ShapeDtypeStruct((dim, tok), F32),
            jax.ShapeDtypeStruct((dim, rows), BF16),
            jax.ShapeDtypeStruct((dim, tokens), BF16),
        ],
        scratch_shapes=[
            pltpu.VMEM((n, rows, tok), BF16),
            pltpu.VMEM((2, dim, tok), F32),
            pltpu.VMEM((chips, dim, tok), F32),
            pltpu.VMEM((chips, dim, tok), F32),
            pltpu.VMEM((chips, dim, tok), F32),
            dma((3,)), dma((2, 2)), dma((2,)), dma((chips,)), dma((16,)), dma((16,)), dma((2,)), dma((2,)),
        ],
        compiler_params=pltpu.CompilerParams(vmem_limit_bytes=63 * MIB, collective_id=1, has_side_effects=True),
        cost_estimate=cost(6 * n * tok * dim * rows, 6 * n * tok * rows),
        name='grad',
    )(e, wt, x, at, upt, down, cm, gs, lab)


def solution(mesh):
    n = mesh.shape['stage']
    row_spec = P(('data', 'stage'), None)
    vocab_spec = P('stage', None)
    layer_spec = P('stage', None, None, None)
    acts_spec = P(('data', 'stage'), None, None)

    def per_device(x_loc, w_loc, labels, loss_mask, e_loc, next_ids, acts_loc, up_loc, down_loc):
        tok = x_loc.shape[0]
        offset = lax.axis_index('stage') * w_loc.shape[0]
        wt, at, down = w_loc.T, acts_loc[0].T, jnp.swapaxes(down_loc[0], 1, 2)
        ids = (next_ids - offset).reshape(n, 1, tok)
        lab = (labels - offset).reshape(n, 1, tok)
        mask = loss_mask.astype(F32).reshape(n, 1, tok)
        x, hsum, y0, upt = gather(x_loc.T, ids, e_loc.T, up_loc[0], down, at)
        e, cm, st, embed_rows = logits(wt, x, lab, hsum)
        gs, loss, y1 = stats(st, mask, at, upt, down)
        dx, dw, y2 = grad(wt, e, x, at, upt, down, cm, gs, lab)
        stage_out = jnp.concatenate([y0, y1, y2], axis=1)
        return loss[0, :1], dx.T, dw.T, embed_rows.T, stage_out.T[None]

    return jax.shard_map(
        per_device,
        mesh=mesh,
        in_specs=(row_spec, vocab_spec, P('data'), P('data'), vocab_spec, P('data'), acts_spec, layer_spec, layer_spec),
        out_specs=(P('data'), row_spec, row_spec, row_spec, acts_spec),
        check_vma=False,
    )
```

```python
import functools

import jax
import jax.numpy as jnp
from jax import lax
from jax.experimental import pallas as pl
from jax.experimental.pallas import tpu as pltpu
from jax.sharding import PartitionSpec as P

F32 = jnp.float32
BF16 = jnp.bfloat16
MESH = pl.DeviceIdType.MESH
CHUNK = 384
GROUP = 2
MIB = 1024 * 1024


def mm(a, b, ca, cb):
    return lax.dot_general(a, b, (((ca,), (cb,)), ((), ())), preferred_element_type=F32)


def params(limit, **kw):
    return pltpu.CompilerParams(vmem_limit_bytes=limit * MIB, **kw)


def cost(flops, nbytes):
    return pl.CostEstimate(flops=int(flops), bytes_accessed=int(nbytes), transcendentals=0)


def transpose_into(dst_ref, src, step):
    for c in range(0, src.shape[1], step):
        dst_ref[pl.ds(c, step), :] = src[:, c:c + step].T


def side_by_side(ref):
    return jnp.concatenate([ref[b] for b in range(ref.shape[0])], axis=1)


def gelu(x):
    k = 0.7978845608028654
    inner = x * (k + (k * 0.044715) * (x * x))
    half = 0.5 * x
    return half + half * jnp.tanh(inner)


MLP_TILE = 512
MLP_GATHER = 2
MLP_STATS = 3


def mlp_layer(h, upt, down):
    hidden = upt.shape[0]
    u = jnp.concatenate(
        [gelu(mm(upt[pl.ds(c, 512), :], h, 1, 0)).astype(BF16) for c in range(0, hidden, 512)], axis=0)
    return (h.astype(F32) + mm(down[...], u, 1, 0)).astype(BF16)


def is_middle():
    stage = lax.axis_index('stage')
    return (stage > 0) & (stage < lax.axis_size('stage') - 1)


class Place:
    def __init__(self, n):
        stage = lax.axis_index('stage')
        self.chips = n // 2
        self.far = self.chips // 2
        self.z, self.core = stage // 2, lax.rem(stage, 2)
        self.partner = {'stage': 2 * self.z + 1 - self.core}
        self.along = [{'stage': 2 * self.chip(1) + self.core}, {'stage': 2 * self.chip(-1) + self.core}]

    def chip(self, steps):
        return lax.rem(self.z + steps + self.chips, self.chips)

    def block(self, chip, own_side):
        return 2 * chip + (self.core if own_side else 1 - self.core)

    def hail(self, barrier):
        for peer in [self.partner] + self.along:
            pl.semaphore_signal(barrier, inc=1, device_id=peer, device_id_type=MESH)


def gather_kernel(n, x_ref, ids_ref, et_hbm, up_hbm, down_hbm, a_hbm, x_out, h_out, y_out, upt_out, x_all, et, up_buf, upt_buf,
                  down_buf, a_buf, y_buf, send_buf, own, pair, load_sem, out_sem, ring_send, ring_recv, side_send, side_recv,
                  pair_send, pair_recv):
    here = Place(n)
    dim, tok = x_ref.shape
    half = dim // 2
    rows = et.shape[1]
    layers = up_buf.shape[0]
    mine = here.block(here.z, True)
    loads = [
        pltpu.make_async_copy(src, dst, load_sem.at[k])
        for k, (src, dst) in enumerate([
            (up_hbm, up_buf), (down_hbm, down_buf), (a_hbm.at[:, pl.ds(0, MLP_GATHER * MLP_TILE)], a_buf), (et_hbm, et),
            (x_ref, x_all.at[mine])])
    ]
    for load in loads:
        load.start()
    barrier = pltpu.get_barrier_semaphore()
    here.hail(barrier)
    pl.semaphore_wait(barrier, 3)

    def unit(way, k, h):
        sl = pl.ds(h * half, half)
        block = here.block(here.chip(k if way else -k), True)
        src = x_ref.at[sl, :] if k == 0 else x_all.at[block, sl, :]
        s = way * 8 + k * 2 + h
        return pltpu.make_async_remote_copy(
            src_ref=src, dst_ref=x_all.at[block, sl, :], send_sem=ring_send.at[s], recv_sem=ring_recv.at[s],
            device_id=here.along[way], device_id_type=MESH)

    def side(way, k, h):
        sl = pl.ds(h * half, half)
        block = here.block(here.chip(1 + k if way else -1 - k), True)
        s = way * 8 + k * 2 + h
        return pltpu.make_async_remote_copy(
            src_ref=x_all.at[block, sl, :], dst_ref=x_all.at[block, sl, :], send_sem=side_send.at[s], recv_sem=side_recv.at[s],
            device_id=here.partner, device_id_type=MESH)

    def side_mine():
        return pltpu.make_async_remote_copy(
            src_ref=x_ref, dst_ref=x_all.at[mine], send_sem=side_send.at[16], recv_sem=side_recv.at[16],
            device_id=here.partner, device_id_type=MESH)

    last = here.far - 1
    arrivals = [[(k, h) for k in range(last) for h in range(2)] + [(last, way)] for way in range(2)]

    def event(u):
        for way in range(2):
            k, h = arrivals[way][u]
            unit(way, k, h).wait_recv()
            if (k + 1, h) in arrivals[way]:
                unit(way, k + 1, h).start()
            side(way, k, h).start()

    for h in range(2):
        for way in range(2):
            unit(way, 0, h).start()
    side_mine().start()

    def pair_copy(i):
        return pltpu.make_async_remote_copy(
            src_ref=send_buf.at[lax.rem(i, 2)], dst_ref=pair.at[i], send_sem=pair_send.at[lax.rem(i, 2)],
            recv_sem=pair_recv.at[i], device_id=here.partner, device_id_type=MESH)

    def pair_add(i):
        pair_copy(i).wait_recv()
        own[i] = (own[i].astype(F32) + pair[i].astype(F32)).astype(BF16)

    loads[0].wait()
    for i in range(layers):
        transpose_into(upt_buf.at[i], up_buf[i], 256)
    loads[1].wait()
    loads[2].wait()
    def tiles(m, carry):
        cols = pl.ds(pl.multiple_of(m * MLP_TILE, MLP_TILE), MLP_TILE)

        @pl.when(is_middle())
        def _():
            h = a_buf[:, cols]
            for i in range(layers):
                h = mlp_layer(h, upt_buf.at[i], down_buf.at[i])
            y_buf[:, cols] = h

        @pl.when(jnp.logical_not(is_middle()))
        def _():
            y_buf[:, cols] = a_buf[:, cols]
        return carry

    lax.fori_loop(0, 1, tiles, 0)
    event(0)
    loads[3].wait()
    index = lax.broadcasted_iota(jnp.int32, (rows, 2 * tok), 0)

    def embed(i, carry):
        @pl.when(i >= 2)
        def _():
            pair_copy(i - 2).wait_send()

        ids = jnp.concatenate([ids_ref[here.block(i, False)], ids_ref[here.block(i, True)]], axis=1)
        hot = jnp.where(index == ids, 1.0, 0.0).astype(BF16)
        out = mm(et[...], hot, 1, 0).astype(BF16)
        send_buf[lax.rem(i, 2)] = out[:, :tok]
        own[i] = out[:, tok:]
        pair_copy(i).start()

        @pl.when(i >= 1)
        def _():
            pair_add(i - 1)

        for u, at in enumerate([0, 2, 3, 5, 6]):
            @pl.when(i == at)
            def _():
                event(u + 1)
        return carry

    lax.fori_loop(0, here.chips, embed, 0)
    event(here.chips - 2)
    pair_add(here.chips - 1)
    outs = [
        pltpu.make_async_copy(src, dst, out_sem.at[k])
        for k, (src, dst) in enumerate([(own, h_out), (upt_buf, upt_out), (x_all, x_out), (y_buf, y_out.at[:, pl.ds(0, MLP_GATHER * MLP_TILE)])])
    ]
    outs[0].start()
    outs[1].start()
    loads[4].wait()
    side_mine().wait()
    for way in range(2):
        for k, h in arrivals[way]:
            side(way, k, h).wait()
    outs[2].start()
    lax.fori_loop(1, MLP_GATHER, tiles, 0)
    outs[3].start()
    for way in range(2):
        for k, h in arrivals[way]:
            unit(way, k, h).wait_send()
    for i in range(here.chips - 2, here.chips):
        pair_copy(i).wait_send()
    for out in outs:
        out.wait()


def gather(xt, ids, et, up, down, at):
    dim, tok = xt.shape
    n = ids.shape[0]
    rows = et.shape[1]
    layers, _, hidden = up.shape
    tokens = MLP_GATHER * MLP_TILE
    vmem = pl.BlockSpec(memory_space=pltpu.VMEM)
    anywhere = pl.BlockSpec(memory_space=pl.ANY)
    dma = pltpu.SemaphoreType.DMA
    return pl.pallas_call(
        functools.partial(gather_kernel, n),
        in_specs=[vmem, vmem] + [anywhere] * 4,
        out_specs=[anywhere] * 4,
        out_shape=[
            jax.ShapeDtypeStruct((n, dim, tok), BF16),
            jax.ShapeDtypeStruct((n // 2, dim, tok), BF16),
            jax.ShapeDtypeStruct(at.shape, BF16),
            jax.ShapeDtypeStruct((layers, hidden, dim), BF16),
        ],
        scratch_shapes=[
            pltpu.VMEM((n, dim, tok), BF16),
            pltpu.VMEM((dim, rows), BF16),
            pltpu.VMEM((layers, dim, hidden), BF16),
            pltpu.VMEM((layers, hidden, dim), BF16),
            pltpu.VMEM((layers, dim, hidden), BF16),
            pltpu.VMEM((dim, tokens), BF16),
            pltpu.VMEM((dim, tokens), BF16),
            pltpu.VMEM((2, dim, tok), BF16),
            pltpu.VMEM((n // 2, dim, tok), BF16),
            pltpu.VMEM((n // 2, dim, tok), BF16),
            dma((5,)), dma((4,)), dma((16,)), dma((16,)), dma((17,)), dma((17,)), dma((2,)), dma((n // 2,)),
        ],
        compiler_params=params(56, collective_id=2, has_side_effects=True),
        cost_estimate=cost(2 * n * tok * dim * rows, 4 * n * tok * dim),
        name='gather',
    )(xt, ids, et, up, down, at)


def logits_kernel(n, wt_ref, x_ref, lab_ref, h_hbm, e_ref, cm_ref, st_ref, h_ref, w_ref, own, chain, load_sem, chain_send, chain_recv):
    here = Place(n)
    far = here.far
    half = h_ref.shape[0] // 2
    step = pl.program_id(0)
    load = pltpu.make_async_copy(h_hbm, own, load_sem.at[0])

    @pl.when(step == 0)
    def _():
        load.start()
        here.hail(pltpu.get_barrier_semaphore())

    def target_chip(way, k):
        return here.chip(far - k if way == 0 else k - far)

    def unit(way, k, h, src):
        sl = pl.ds(h * half, half)
        s = way * 8 + k * 2 + h
        return pltpu.make_async_remote_copy(
            src_ref=src.at[sl, :], dst_ref=chain.at[way * far + k, sl, :], send_sem=chain_send.at[s], recv_sem=chain_recv.at[s],
            device_id=here.along[way], device_id_type=MESH)

    def forward(way, k, h):
        arrived = chain.at[way * far + k]
        unit(way, k, h, arrived).wait_recv()
        sl = pl.ds(h * half, half)
        arrived[sl, :] = (arrived[sl, :].astype(F32) + own[target_chip(way, k + 1), sl, :].astype(F32)).astype(BF16)
        unit(way, k + 1, h, arrived).start()

    rows = wt_ref.shape[1]
    tok = x_ref.shape[2]

    @pl.when(pl.program_id(0) == 0)
    def _():
        transpose_into(w_ref, wt_ref, 256)

    x = side_by_side(x_ref)
    lab = side_by_side(lab_ref)
    index = lax.broadcasted_iota(jnp.int32, (CHUNK, GROUP * tok), 0)
    maxes, sums = [], []
    target = jnp.zeros((1, GROUP * tok), F32)
    for c in range(rows // CHUNK):
        sl = pl.ds(c * CHUNK, CHUNK)
        z = mm(w_ref[sl, :], x, 1, 0)
        m = jnp.max(z, axis=0, keepdims=True)
        e = jnp.exp(z - m)
        for b in range(GROUP):
            e_ref[b, sl, :] = e[:, b * tok:(b + 1) * tok]
        maxes.append(m)
        sums.append(jnp.sum(e, axis=0, keepdims=True))
        target += jnp.sum(jnp.where(index == lab - c * CHUNK, z, 0.0), axis=0, keepdims=True)
    m = functools.reduce(jnp.maximum, maxes)
    s = sum(si * jnp.exp(mi - m) for mi, si in zip(maxes, sums))
    cm = jnp.concatenate(maxes, axis=0)
    st = jnp.concatenate([m, s, target, jnp.zeros((5, GROUP * tok), F32)], axis=0)
    for b in range(GROUP):
        cm_ref[b] = cm[:, b * tok:(b + 1) * tok]
        st_ref[b] = st[:, b * tok:(b + 1) * tok]

    @pl.when(step == 0)
    def _():
        pl.semaphore_wait(pltpu.get_barrier_semaphore(), 3)
        load.wait()
        for way in range(2):
            unit(way, 0, way, own.at[target_chip(way, 0)]).start()
        for way in range(2):
            unit(way, 1, 1 - way, own.at[target_chip(way, 1)]).start()

    @pl.when(step == 2)
    def _():
        for way in range(2):
            forward(way, 0, way)
        for way in range(2):
            forward(way, 1, 1 - way)

    @pl.when(step == 4)
    def _():
        for way in range(2):
            forward(way, 1, way)
        for way in range(2):
            forward(way, 2, 1 - way)

    @pl.when(step == 6)
    def _():
        for way in range(2):
            forward(way, 2, way)

    @pl.when(step == 7)
    def _():
        for h in range(2):
            for way in range(2):
                unit(way, far - 1, h, own.at[0]).wait_recv()
        total = own[here.z].astype(F32) + (chain[far - 1].astype(F32) + chain[2 * far - 1].astype(F32))
        h_ref[...] = total.astype(BF16)
        for way in range(2):
            for k in range(far):
                for h in range(2):
                    if k > 0 or h == way:
                        unit(way, k, h, own.at[0]).wait_send()


def logits(wt, x, lab, hsum):
    dim, rows = wt.shape
    n, _, tok = x.shape
    block = lambda r, c: pl.BlockSpec((GROUP, r, c), lambda i: (i, 0, 0))
    dma = pltpu.SemaphoreType.DMA
    return pl.pallas_call(
        functools.partial(logits_kernel, n),
        grid=(n // GROUP,),
        in_specs=[
            pl.BlockSpec((dim, rows), lambda i: (0, 0)), block(dim, tok), block(1, tok), pl.BlockSpec(memory_space=pl.ANY)],
        out_specs=[block(rows, tok), block(8, tok), block(8, tok), pl.BlockSpec((dim, tok), lambda i: (0, 0))],
        out_shape=[
            jax.ShapeDtypeStruct((n, rows, tok), F32),
            jax.ShapeDtypeStruct((n, 8, tok), F32),
            jax.ShapeDtypeStruct((n, 8, tok), F32),
            jax.ShapeDtypeStruct((dim, tok), BF16),
        ],
        scratch_shapes=[
            pltpu.VMEM((rows, dim), BF16), pltpu.VMEM(hsum.shape, BF16), pltpu.VMEM(hsum.shape, BF16),
            dma((1,)), dma((16,)), dma((16,)),
        ],
        compiler_params=params(56, collective_id=3, has_side_effects=True),
        cost_estimate=cost(2 * n * tok * dim * rows, 4 * n * tok * rows),
        name='logits',
    )(wt, x, lab, hsum)


def stats_kernel(n, st_ref, mask_ref, a_hbm, upt_hbm, down_hbm, y_in, out_ref, loss_ref, y_hbm, got, every, upt_buf, down_buf, a_buf,
                 y_buf, send1, recv1, send2, recv2, load_sem, a_sem, y_sem):
    me = lax.axis_index('stage')
    layers = upt_buf.shape[0]
    loads = [
        pltpu.make_async_copy(src, dst, load_sem.at[k])
        for k, (src, dst) in enumerate([(upt_hbm, upt_buf), (down_hbm, down_buf)])
    ]
    for load in loads:
        load.start()

    def load_a(m):
        start = pl.multiple_of((m + MLP_GATHER) * MLP_TILE, MLP_TILE)
        slot = lax.rem(m, 2)
        return pltpu.make_async_copy(a_hbm.at[:, pl.ds(start, MLP_TILE)], a_buf.at[slot], a_sem.at[slot])

    def store_y(m):
        slot = lax.rem(m, 2)
        start = pl.multiple_of((m + MLP_GATHER) * MLP_TILE, MLP_TILE)
        return pltpu.make_async_copy(y_buf.at[slot], y_hbm.at[:, pl.ds(start, MLP_TILE)], y_sem.at[slot])

    load_a(0).start()
    barrier = pltpu.get_barrier_semaphore()
    peers = [lax.rem(me + d, n) for d in range(n)]
    for d in range(1, n):
        pl.semaphore_signal(barrier, inc=1, device_id={'stage': peers[d]}, device_id_type=MESH)
    pl.semaphore_wait(barrier, n - 1)

    first = []
    for d in range(1, n):
        first.append(pltpu.make_async_remote_copy(
            src_ref=st_ref.at[peers[d]], dst_ref=got.at[d], send_sem=send1.at[d], recv_sem=recv1.at[d],
            device_id={'stage': peers[d]}, device_id_type=MESH))
        first[-1].start()

    weight = mask_ref[...]
    count = jnp.maximum(jnp.sum(weight, keepdims=True)[0], 1.0)
    second = [
        pltpu.make_async_remote_copy(
            src_ref=every.at[me], dst_ref=every.at[me], send_sem=send2.at[d], recv_sem=recv2.at[d],
            device_id={'stage': peers[d]}, device_id_type=MESH)
        for d in range(1, n)
    ]

    def reduce_stats():
        for copy in first:
            copy.wait()
        parts = [st_ref[me]] + [got[d] for d in range(1, n)]
        m = functools.reduce(jnp.maximum, [p[0:1] for p in parts])
        total = sum(p[1:2] * jnp.exp(p[0:1] - m) for p in parts)
        target = sum(p[2:3] for p in parts)
        w = mask_ref[me]
        scale = w / count
        term = w * (jnp.log(total) + m - target)
        every[me] = jnp.concatenate([m, scale / total, scale, term, jnp.zeros((4, m.shape[1]), F32)], axis=0)

    for load in loads:
        load.wait()
    tiles = MLP_STATS

    def piece(q, carry):
        m, i = q // layers, lax.rem(q, layers)
        slot = lax.rem(m, 2)

        @pl.when(i == 0)
        def _():
            @pl.when(m < tiles - 1)
            def _():
                load_a(m + 1).start()

            load_a(m).wait()

            @pl.when(m >= 2)
            def _():
                store_y(m - 2).wait()

            y_buf[slot] = a_buf[slot]

        @pl.when(is_middle())
        def _():
            y_buf[slot] = mlp_layer(y_buf[slot], upt_buf.at[i], down_buf.at[i])

        @pl.when(i == layers - 1)
        def _():
            store_y(m).start()

        @pl.when(q == 1)
        def _():
            reduce_stats()
            for copy in second:
                copy.start()

        return carry

    lax.fori_loop(0, tiles * layers, piece, 0)
    for copy in second:
        copy.wait()
    out_ref[...] = every[...]
    loss_ref[...] = jnp.broadcast_to(jnp.sum(every[:, 3, :], keepdims=True) / count, loss_ref.shape)
    for m in range(tiles - 2, tiles):
        store_y(m).wait()


def stats(st, mask, at, upt, down, y):
    n, _, tok = st.shape
    dim = at.shape[0]
    vmem = pl.BlockSpec(memory_space=pltpu.VMEM)
    anywhere = pl.BlockSpec(memory_space=pl.ANY)
    dma = pltpu.SemaphoreType.DMA
    return pl.pallas_call(
        functools.partial(stats_kernel, n),
        in_specs=[vmem, vmem] + [anywhere] * 4,
        out_specs=[vmem, vmem, anywhere],
        out_shape=[
            jax.ShapeDtypeStruct((n, 8, tok), F32),
            jax.ShapeDtypeStruct((8, 128), F32),
            jax.ShapeDtypeStruct(y.shape, BF16),
        ],
        scratch_shapes=[
            pltpu.VMEM((n, 8, tok), F32),
            pltpu.VMEM((n, 8, tok), F32),
            pltpu.VMEM(upt.shape, BF16),
            pltpu.VMEM(down.shape, BF16),
            pltpu.VMEM((2, dim, MLP_TILE), BF16),
            pltpu.VMEM((2, dim, MLP_TILE), BF16),
            dma((n,)), dma((n,)), dma((n,)), dma((n,)), dma((2,)), dma((2,)), dma((2,)),
        ],
        input_output_aliases={5: 2},
        compiler_params=params(56, collective_id=0, has_side_effects=True),
        cost_estimate=cost(3e10, 2e7),
        name='stats',
    )(st, mask, at, upt, down, y)


def grad_kernel(n, e_hbm, w_hbm, x_hbm, a_hbm, upt_hbm, down_hbm, y_in, cm_ref, gs_ref, lab_ref, dx_ref, dw_hbm, y_hbm, g_buf, send_buf,
                own, pair, chain, load_sem, e_sem, pair_send, pair_recv, chain_send, chain_recv, a_sem, y_sem):
    stage = lax.axis_index('stage')
    chips = n // 2
    far = chips // 2
    z, core = stage // 2, lax.rem(stage, 2)
    dim, tok = dx_ref.shape
    rows = w_hbm.shape[1]
    half = dim // 2
    partner = {'stage': 2 * z + 1 - core}
    ahead = {'stage': 2 * lax.rem(z + 1, chips) + core}
    behind = {'stage': 2 * lax.rem(z + chips - 1, chips) + core}

    def chip_at(i):
        size = far - (i + 1) // 2
        sign = 2 * lax.rem(i, 2) - 1
        return lax.rem(z + sign * size + chips, chips)

    def block_at(i, own_side):
        return 2 * chip_at(i) + (core if own_side else 1 - core)

    def pair_copy(i):
        return pltpu.make_async_remote_copy(
            src_ref=send_buf.at[lax.rem(i, 2)], dst_ref=pair.at[i], send_sem=pair_send.at[lax.rem(i, 2)],
            recv_sem=pair_recv.at[i], device_id=partner, device_id_type=MESH)

    def pair_add(i):
        pair_copy(i).wait_recv()
        own[i] += pair[i]

    def unit(way, k, h, src):
        sl = pl.ds(h * half, half)
        s = way * 8 + k * 2 + h
        return pltpu.make_async_remote_copy(
            src_ref=src.at[sl, :], dst_ref=chain.at[way * far + k, sl, :], send_sem=chain_send.at[s], recv_sem=chain_recv.at[s],
            device_id=ahead if way == 0 else behind, device_id_type=MESH)

    def place(way, k):
        return 0 if k == 0 else 2 * k - 1 + way

    def first_send(way):
        unit(way, 0, way, own.at[0]).start()

    def plain_send(way):
        unit(way, 1, 1 - way, own.at[place(way, 1)]).start()

    def forward(way, k, h):
        here = chain.at[way * far + k]
        unit(way, k, h, here).wait_recv()
        sl = pl.ds(h * half, half)
        here[sl, :] += own[place(way, k + 1), sl, :]
        unit(way, k + 1, h, here).start()

    def gradients(w_buf, e_buf):
        def load_e(i, q):
            slot = lax.rem(i, 2)
            return pltpu.make_async_copy(e_hbm.at[block_at(i, q == 1)], e_buf.at[slot, q], e_sem.at[slot, q])

        for q in range(2):
            load_e(0, q).start()
        load_w = pltpu.make_async_copy(w_hbm, w_buf, load_sem.at[0])
        load_w.start()
        barrier = pltpu.get_barrier_semaphore()
        for peer in (partner, ahead, behind):
            pl.semaphore_signal(barrier, inc=1, device_id=peer, device_id_type=MESH)
        pl.semaphore_wait(barrier, 3)
        index = lax.broadcasted_iota(jnp.int32, (CHUNK, tok), 0)
        load_w.wait()

        def body(i, carry):
            @pl.when(i < chips - 1)
            def _():
                for q in range(2):
                    load_e(i + 1, q).start()

            @pl.when(i >= 2)
            def _():
                pair_copy(i - 2).wait_send()

            for q in range(2):
                load_e(i, q).wait()
            slot = lax.rem(i, 2)
            blocks = [block_at(i, q == 1) for q in range(2)]
            parts = [[], []]
            for q in range(2):
                gs, cm, lab = gs_ref[blocks[q]], cm_ref[blocks[q]], lab_ref[blocks[q]]
                m, over, scale = gs[0:1], gs[1:2], gs[2:3]
                for c in range(rows // CHUNK):
                    sl = pl.ds(c * CHUNK, CHUNK)
                    p = e_buf[slot, q, sl, :] * (jnp.exp(cm[c:c + 1] - m) * over)
                    g = jnp.where(index == lab - c * CHUNK, p - scale, p).astype(BF16)
                    g_buf[blocks[q], sl, :] = g
                    parts[q].append(g)
            both = jnp.concatenate([jnp.concatenate(p, axis=0) for p in parts], axis=1)
            dx = mm(w_buf[...], both, 1, 0)
            send_buf[slot] = dx[:, :tok]
            own[i] = dx[:, tok:]
            pair_copy(i).start()

            @pl.when(i >= 1)
            def _():
                pair_add(i - 1)

            @pl.when(i == 1)
            def _():
                first_send(0)
                first_send(1)

            @pl.when(i == 2)
            def _():
                plain_send(0)

            @pl.when(i == 3)
            def _():
                plain_send(1)

            @pl.when(i == chips - 2)
            def _():
                for way in range(2):
                    forward(way, 0, way)
            return carry

        lax.fori_loop(0, chips, body, 0)

    pl.run_scoped(gradients, pltpu.VMEM((dim, rows), BF16), pltpu.VMEM((2, 2, rows, tok), F32))
    pair_add(chips - 1)

    def fill(x_buf, upt_buf, down_buf, a_buf, y_buf, dw_buf):
        loads = [
            pltpu.make_async_copy(src, dst, load_sem.at[k])
            for k, (src, dst) in enumerate([(x_hbm, x_buf), (upt_hbm, upt_buf), (down_hbm, down_buf)])
        ]
        for load in loads:
            load.start()
        done = MLP_GATHER + MLP_STATS
        tiles = y_hbm.shape[1] // MLP_TILE - done

        def cols(m):
            return pl.ds(pl.multiple_of(m * MLP_TILE, MLP_TILE), MLP_TILE)

        def load_a(m):
            slot = lax.rem(m, 2)
            return pltpu.make_async_copy(a_hbm.at[:, cols(m + done)], a_buf.at[slot], a_sem.at[slot])

        def store_y(m):
            slot = lax.rem(m, 2)
            return pltpu.make_async_copy(y_buf.at[slot], y_hbm.at[:, cols(m + done)], y_sem.at[slot])

        load_a(0).start()
        loads[0].wait()
        width = 512
        pieces = rows // width

        def store_dw(j):
            slot = lax.rem(j, 2)
            start = pl.multiple_of(j * width, width)
            return pltpu.make_async_copy(dw_buf.at[slot], dw_hbm.at[:, pl.ds(start, width)], y_sem.at[slot])

        def head(j, carry):
            start = pl.multiple_of(j * width, width)
            g = jnp.concatenate([g_buf[b, pl.ds(start, width), :] for b in range(n)], axis=1)

            @pl.when(j >= 2)
            def _():
                store_dw(j - 2).wait()

            dw_buf[lax.rem(j, 2)] = mm(side_by_side(x_buf), g, 1, 1).astype(BF16)
            store_dw(j).start()

            @pl.when(j == 0)
            def _():
                for way in range(2):
                    forward(way, 1, 1 - way)

            @pl.when(j == 2)
            def _():
                for way in range(2):
                    forward(way, 1, way)

            @pl.when(j == 4)
            def _():
                for way in range(2):
                    forward(way, 2, 1 - way)

            @pl.when(j == pieces - 1)
            def _():
                for way in range(2):
                    forward(way, 2, way)
            return carry

        lax.fori_loop(0, pieces, head, 0)
        for j in range(pieces - 2, pieces):
            store_dw(j).wait()
        loads[1].wait()
        loads[2].wait()

        def layers(m, carry):
            slot = lax.rem(m, 2)

            @pl.when(m < tiles - 1)
            def _():
                load_a(m + 1).start()

            load_a(m).wait()

            @pl.when(m >= 2)
            def _():
                store_y(m - 2).wait()

            @pl.when(is_middle())
            def _():
                h = a_buf[slot]
                for i in range(upt_buf.shape[0]):
                    h = mlp_layer(h, upt_buf.at[i], down_buf.at[i])
                y_buf[slot] = h

            @pl.when(jnp.logical_not(is_middle()))
            def _():
                y_buf[slot] = a_buf[slot]

            store_y(m).start()
            return carry

        lax.fori_loop(0, tiles, layers, 0)
        for m in range(tiles - 2, tiles):
            store_y(m).wait()

    pl.run_scoped(
        fill, pltpu.VMEM(x_hbm.shape, BF16), pltpu.VMEM(upt_hbm.shape, BF16), pltpu.VMEM(down_hbm.shape, BF16),
        pltpu.VMEM((2, dim, MLP_TILE), BF16), pltpu.VMEM((2, dim, MLP_TILE), BF16), pltpu.VMEM((2, dim, 512), BF16))
    for h in range(2):
        for way in range(2):
            unit(way, far - 1, h, own.at[0]).wait_recv()
    dx_ref[...] = own[chips - 1] + (chain[far - 1] + chain[2 * far - 1])
    for i in range(chips - 2, chips):
        pair_copy(i).wait_send()
    for way in range(2):
        for k in range(far):
            for h in range(2):
                if k > 0 or h == way:
                    unit(way, k, h, own.at[0]).wait_send()


def grad(wt, e, x, at, upt, down, y, cm, gs, lab):
    dim, rows = wt.shape
    n, _, tok = e.shape
    chips = n // 2
    vmem = pl.BlockSpec(memory_space=pltpu.VMEM)
    anywhere = pl.BlockSpec(memory_space=pl.ANY)
    dma = pltpu.SemaphoreType.DMA
    return pl.pallas_call(
        functools.partial(grad_kernel, n),
        in_specs=[anywhere] * 7 + [vmem] * 3,
        out_specs=[vmem, anywhere, anywhere],
        out_shape=[
            jax.ShapeDtypeStruct((dim, tok), F32),
            jax.ShapeDtypeStruct((dim, rows), BF16),
            jax.ShapeDtypeStruct(y.shape, BF16),
        ],
        scratch_shapes=[
            pltpu.VMEM((n, rows, tok), BF16),
            pltpu.VMEM((2, dim, tok), F32),
            pltpu.VMEM((chips, dim, tok), F32),
            pltpu.VMEM((chips, dim, tok), F32),
            pltpu.VMEM((chips, dim, tok), F32),
            dma((3,)), dma((2, 2)), dma((2,)), dma((chips,)), dma((16,)), dma((16,)), dma((2,)), dma((2,)),
        ],
        input_output_aliases={6: 2},
        compiler_params=pltpu.CompilerParams(vmem_limit_bytes=63 * MIB, collective_id=1, has_side_effects=True),
        cost_estimate=cost(6 * n * tok * dim * rows, 6 * n * tok * rows),
        name='grad',
    )(e, wt, x, at, upt, down, y, cm, gs, lab)


def solution(mesh):
    n = mesh.shape['stage']
    row_spec = P(('data', 'stage'), None)
    vocab_spec = P('stage', None)
    layer_spec = P('stage', None, None, None)
    acts_spec = P(('data', 'stage'), None, None)

    def per_device(x_loc, w_loc, labels, loss_mask, e_loc, next_ids, acts_loc, up_loc, down_loc):
        tok = x_loc.shape[0]
        offset = lax.axis_index('stage') * w_loc.shape[0]
        wt, at, down = w_loc.T, acts_loc[0].T, jnp.swapaxes(down_loc[0], 1, 2)
        ids = (next_ids - offset).reshape(n, 1, tok)
        lab = (labels - offset).reshape(n, 1, tok)
        mask = loss_mask.astype(F32).reshape(n, 1, tok)
        x, hsum, y, upt = gather(x_loc.T, ids, e_loc.T, up_loc[0], down, at)
        e, cm, st, embed_rows = logits(wt, x, lab, hsum)
        gs, loss, y = stats(st, mask, at, upt, down, y)
        dx, dw, stage_out = grad(wt, e, x, at, upt, down, y, cm, gs, lab)
        return loss[0, :1], dx.T, dw.T, embed_rows.T, stage_out.T[None]

    return jax.shard_map(
        per_device,
        mesh=mesh,
        in_specs=(row_spec, vocab_spec, P('data'), P('data'), vocab_spec, P('data'), acts_spec, layer_spec, layer_spec),
        out_specs=(P('data'), row_spec, row_spec, row_spec, acts_spec),
        check_vma=False,
    )
```

```python
import functools

import jax
import jax.numpy as jnp
from jax import lax
from jax.experimental import pallas as pl
from jax.experimental.pallas import tpu as pltpu
from jax.sharding import PartitionSpec as P

F32 = jnp.float32
BF16 = jnp.bfloat16
MESH = pl.DeviceIdType.MESH
CHUNK = 384
GROUP = 2
MIB = 1024 * 1024


def mm(a, b, ca, cb):
    return lax.dot_general(a, b, (((ca,), (cb,)), ((), ())), preferred_element_type=F32)


def params(limit, **kw):
    return pltpu.CompilerParams(vmem_limit_bytes=limit * MIB, **kw)


def cost(flops, nbytes):
    return pl.CostEstimate(flops=int(flops), bytes_accessed=int(nbytes), transcendentals=0)


def transpose_into(dst_ref, src, step):
    for c in range(0, src.shape[1], step):
        dst_ref[pl.ds(c, step), :] = src[:, c:c + step].T


def side_by_side(ref):
    return jnp.concatenate([ref[b] for b in range(ref.shape[0])], axis=1)


def gelu(x):
    k = 0.7978845608028654
    inner = x * (k + (k * 0.044715) * (x * x))
    half = 0.5 * x
    return half + half * jnp.tanh(inner)


MLP_TILE = 512
MLP_GATHER = 2
MLP_STATS = 3


def mlp_layer(h, upt, down):
    hidden = upt.shape[0]
    u = jnp.concatenate(
        [gelu(mm(upt[pl.ds(c, 512), :], h, 1, 0)).astype(BF16) for c in range(0, hidden, 512)], axis=0)
    return (h.astype(F32) + mm(down[...], u, 1, 0)).astype(BF16)


def is_middle():
    stage = lax.axis_index('stage')
    return (stage > 0) & (stage < lax.axis_size('stage') - 1)


class Place:
    def __init__(self, n):
        stage = lax.axis_index('stage')
        self.chips = n // 2
        self.far = self.chips // 2
        self.z, self.core = stage // 2, lax.rem(stage, 2)
        self.partner = {'stage': 2 * self.z + 1 - self.core}
        self.along = [{'stage': 2 * self.chip(1) + self.core}, {'stage': 2 * self.chip(-1) + self.core}]

    def chip(self, steps):
        return lax.rem(self.z + steps + self.chips, self.chips)

    def block(self, chip, own_side):
        return 2 * chip + (self.core if own_side else 1 - self.core)

    def hail(self, barrier):
        for peer in [self.partner] + self.along:
            pl.semaphore_signal(barrier, inc=1, device_id=peer, device_id_type=MESH)


def gather_kernel(n, x_ref, ids_ref, et_hbm, up_hbm, down_hbm, a_hbm, x_out, h_out, y_out, upt_out, x_all, et, up_buf, upt_buf,
                  down_buf, a_buf, y_buf, send_buf, own, pair, load_sem, out_sem, ring_send, ring_recv, side_send, side_recv,
                  pair_send, pair_recv):
    here = Place(n)
    dim, tok = x_ref.shape
    half = dim // 2
    rows = et.shape[1]
    layers = up_buf.shape[0]
    mine = here.block(here.z, True)
    loads = [
        pltpu.make_async_copy(src, dst, load_sem.at[k])
        for k, (src, dst) in enumerate([
            (up_hbm, up_buf), (down_hbm, down_buf), (a_hbm.at[:, pl.ds(0, MLP_GATHER * MLP_TILE)], a_buf), (et_hbm, et),
            (x_ref, x_all.at[mine])])
    ]
    for load in loads:
        load.start()
    barrier = pltpu.get_barrier_semaphore()
    here.hail(barrier)
    pl.semaphore_wait(barrier, 3)

    def unit(way, k, h):
        sl = pl.ds(h * half, half)
        block = here.block(here.chip(k if way else -k), True)
        src = x_ref.at[sl, :] if k == 0 else x_all.at[block, sl, :]
        s = way * 8 + k * 2 + h
        return pltpu.make_async_remote_copy(
            src_ref=src, dst_ref=x_all.at[block, sl, :], send_sem=ring_send.at[s], recv_sem=ring_recv.at[s],
            device_id=here.along[way], device_id_type=MESH)

    def side(way, k, h):
        sl = pl.ds(h * half, half)
        block = here.block(here.chip(1 + k if way else -1 - k), True)
        s = way * 8 + k * 2 + h
        return pltpu.make_async_remote_copy(
            src_ref=x_all.at[block, sl, :], dst_ref=x_all.at[block, sl, :], send_sem=side_send.at[s], recv_sem=side_recv.at[s],
            device_id=here.partner, device_id_type=MESH)

    def side_mine():
        return pltpu.make_async_remote_copy(
            src_ref=x_ref, dst_ref=x_all.at[mine], send_sem=side_send.at[16], recv_sem=side_recv.at[16],
            device_id=here.partner, device_id_type=MESH)

    last = here.far - 1
    arrivals = [[(k, h) for k in range(last) for h in range(2)] + [(last, way)] for way in range(2)]

    def event(u):
        for way in range(2):
            k, h = arrivals[way][u]
            unit(way, k, h).wait_recv()
            if (k + 1, h) in arrivals[way]:
                unit(way, k + 1, h).start()
            side(way, k, h).start()

    for h in range(2):
        for way in range(2):
            unit(way, 0, h).start()
    side_mine().start()

    def pair_copy(i):
        return pltpu.make_async_remote_copy(
            src_ref=send_buf.at[lax.rem(i, 2)], dst_ref=pair.at[i], send_sem=pair_send.at[lax.rem(i, 2)],
            recv_sem=pair_recv.at[i], device_id=here.partner, device_id_type=MESH)

    def pair_add(i):
        pair_copy(i).wait_recv()
        own[i] = (own[i].astype(F32) + pair[i].astype(F32)).astype(BF16)

    loads[0].wait()
    for i in range(layers):
        transpose_into(upt_buf.at[i], up_buf[i], 256)
    loads[1].wait()
    loads[2].wait()
    def tiles(m, carry):
        cols = pl.ds(pl.multiple_of(m * MLP_TILE, MLP_TILE), MLP_TILE)

        @pl.when(is_middle())
        def _():
            h = a_buf[:, cols]
            for i in range(layers):
                h = mlp_layer(h, upt_buf.at[i], down_buf.at[i])
            y_buf[:, cols] = h

        @pl.when(jnp.logical_not(is_middle()))
        def _():
            y_buf[:, cols] = a_buf[:, cols]
        return carry

    lax.fori_loop(0, 1, tiles, 0)
    event(0)
    loads[3].wait()
    index = lax.broadcasted_iota(jnp.int32, (rows, 2 * tok), 0)

    def embed(i, carry):
        @pl.when(i >= 2)
        def _():
            pair_copy(i - 2).wait_send()

        ids = jnp.concatenate([ids_ref[here.block(i, False)], ids_ref[here.block(i, True)]], axis=1)
        hot = jnp.where(index == ids, 1.0, 0.0).astype(BF16)
        out = mm(et[...], hot, 1, 0).astype(BF16)
        send_buf[lax.rem(i, 2)] = out[:, :tok]
        own[i] = out[:, tok:]
        pair_copy(i).start()

        @pl.when(i >= 1)
        def _():
            pair_add(i - 1)

        for u, at in enumerate([0, 2, 3, 5, 6]):
            @pl.when(i == at)
            def _():
                event(u + 1)
        return carry

    lax.fori_loop(0, here.chips, embed, 0)
    event(here.chips - 2)
    pair_add(here.chips - 1)
    outs = [
        pltpu.make_async_copy(src, dst, out_sem.at[k])
        for k, (src, dst) in enumerate([(own, h_out), (upt_buf, upt_out), (x_all, x_out), (y_buf, y_out)])
    ]
    outs[0].start()
    outs[1].start()
    loads[4].wait()
    side_mine().wait()
    for way in range(2):
        for k, h in arrivals[way]:
            side(way, k, h).wait()
    outs[2].start()
    lax.fori_loop(1, MLP_GATHER, tiles, 0)
    outs[3].start()
    for way in range(2):
        for k, h in arrivals[way]:
            unit(way, k, h).wait_send()
    for i in range(here.chips - 2, here.chips):
        pair_copy(i).wait_send()
    for out in outs:
        out.wait()


def gather(xt, ids, et, up, down, at):
    dim, tok = xt.shape
    n = ids.shape[0]
    rows = et.shape[1]
    layers, _, hidden = up.shape
    tokens = MLP_GATHER * MLP_TILE
    vmem = pl.BlockSpec(memory_space=pltpu.VMEM)
    anywhere = pl.BlockSpec(memory_space=pl.ANY)
    dma = pltpu.SemaphoreType.DMA
    return pl.pallas_call(
        functools.partial(gather_kernel, n),
        in_specs=[vmem, vmem] + [anywhere] * 4,
        out_specs=[anywhere] * 4,
        out_shape=[
            jax.ShapeDtypeStruct((n, dim, tok), BF16),
            jax.ShapeDtypeStruct((n // 2, dim, tok), BF16),
            jax.ShapeDtypeStruct((dim, tokens), BF16),
            jax.ShapeDtypeStruct((layers, hidden, dim), BF16),
        ],
        scratch_shapes=[
            pltpu.VMEM((n, dim, tok), BF16),
            pltpu.VMEM((dim, rows), BF16),
            pltpu.VMEM((layers, dim, hidden), BF16),
            pltpu.VMEM((layers, hidden, dim), BF16),
            pltpu.VMEM((layers, dim, hidden), BF16),
            pltpu.VMEM((dim, tokens), BF16),
            pltpu.VMEM((dim, tokens), BF16),
            pltpu.VMEM((2, dim, tok), BF16),
            pltpu.VMEM((n // 2, dim, tok), BF16),
            pltpu.VMEM((n // 2, dim, tok), BF16),
            dma((5,)), dma((4,)), dma((16,)), dma((16,)), dma((17,)), dma((17,)), dma((2,)), dma((n // 2,)),
        ],
        compiler_params=params(56, collective_id=2, has_side_effects=True),
        cost_estimate=cost(2 * n * tok * dim * rows, 4 * n * tok * dim),
        name='gather',
    )(xt, ids, et, up, down, at)


def logits_kernel(n, wt_ref, x_ref, lab_ref, h_hbm, e_ref, cm_ref, st_ref, h_ref, w_ref, own, chain, load_sem, chain_send, chain_recv):
    here = Place(n)
    far = here.far
    half = h_ref.shape[0] // 2
    step = pl.program_id(0)
    load = pltpu.make_async_copy(h_hbm, own, load_sem.at[0])

    @pl.when(step == 0)
    def _():
        load.start()
        here.hail(pltpu.get_barrier_semaphore())

    def target_chip(way, k):
        return here.chip(far - k if way == 0 else k - far)

    def unit(way, k, h, src):
        sl = pl.ds(h * half, half)
        s = way * 8 + k * 2 + h
        return pltpu.make_async_remote_copy(
            src_ref=src.at[sl, :], dst_ref=chain.at[way * far + k, sl, :], send_sem=chain_send.at[s], recv_sem=chain_recv.at[s],
            device_id=here.along[way], device_id_type=MESH)

    def forward(way, k, h):
        arrived = chain.at[way * far + k]
        unit(way, k, h, arrived).wait_recv()
        sl = pl.ds(h * half, half)
        arrived[sl, :] = (arrived[sl, :].astype(F32) + own[target_chip(way, k + 1), sl, :].astype(F32)).astype(BF16)
        unit(way, k + 1, h, arrived).start()

    rows = wt_ref.shape[1]
    tok = x_ref.shape[2]

    @pl.when(pl.program_id(0) == 0)
    def _():
        transpose_into(w_ref, wt_ref, 256)

    x = side_by_side(x_ref)
    lab = side_by_side(lab_ref)
    index = lax.broadcasted_iota(jnp.int32, (CHUNK, GROUP * tok), 0)
    maxes, sums = [], []
    target = jnp.zeros((1, GROUP * tok), F32)
    for c in range(rows // CHUNK):
        sl = pl.ds(c * CHUNK, CHUNK)
        z = mm(w_ref[sl, :], x, 1, 0)
        m = jnp.max(z, axis=0, keepdims=True)
        e = jnp.exp(z - m)
        for b in range(GROUP):
            e_ref[b, sl, :] = e[:, b * tok:(b + 1) * tok]
        maxes.append(m)
        sums.append(jnp.sum(e, axis=0, keepdims=True))
        target += jnp.sum(jnp.where(index == lab - c * CHUNK, z, 0.0), axis=0, keepdims=True)
    m = functools.reduce(jnp.maximum, maxes)
    s = sum(si * jnp.exp(mi - m) for mi, si in zip(maxes, sums))
    cm = jnp.concatenate(maxes, axis=0)
    st = jnp.concatenate([m, s, target, jnp.zeros((5, GROUP * tok), F32)], axis=0)
    for b in range(GROUP):
        cm_ref[b] = cm[:, b * tok:(b + 1) * tok]
        st_ref[b] = st[:, b * tok:(b + 1) * tok]

    @pl.when(step == 0)
    def _():
        pl.semaphore_wait(pltpu.get_barrier_semaphore(), 3)
        load.wait()
        for way in range(2):
            unit(way, 0, way, own.at[target_chip(way, 0)]).start()
        for way in range(2):
            unit(way, 1, 1 - way, own.at[target_chip(way, 1)]).start()

    @pl.when(step == 2)
    def _():
        for way in range(2):
            forward(way, 0, way)
        for way in range(2):
            forward(way, 1, 1 - way)

    @pl.when(step == 4)
    def _():
        for way in range(2):
            forward(way, 1, way)
        for way in range(2):
            forward(way, 2, 1 - way)

    @pl.when(step == 6)
    def _():
        for way in range(2):
            forward(way, 2, way)

    @pl.when(step == 7)
    def _():
        for h in range(2):
            for way in range(2):
                unit(way, far - 1, h, own.at[0]).wait_recv()
        total = own[here.z].astype(F32) + (chain[far - 1].astype(F32) + chain[2 * far - 1].astype(F32))
        h_ref[...] = total.astype(BF16)
        for way in range(2):
            for k in range(far):
                for h in range(2):
                    if k > 0 or h == way:
                        unit(way, k, h, own.at[0]).wait_send()


def logits(wt, x, lab, hsum):
    dim, rows = wt.shape
    n, _, tok = x.shape
    block = lambda r, c: pl.BlockSpec((GROUP, r, c), lambda i: (i, 0, 0))
    dma = pltpu.SemaphoreType.DMA
    return pl.pallas_call(
        functools.partial(logits_kernel, n),
        grid=(n // GROUP,),
        in_specs=[
            pl.BlockSpec((dim, rows), lambda i: (0, 0)), block(dim, tok), block(1, tok), pl.BlockSpec(memory_space=pl.ANY)],
        out_specs=[block(rows, tok), block(8, tok), block(8, tok), pl.BlockSpec((dim, tok), lambda i: (0, 0))],
        out_shape=[
            jax.ShapeDtypeStruct((n, rows, tok), F32),
            jax.ShapeDtypeStruct((n, 8, tok), F32),
            jax.ShapeDtypeStruct((n, 8, tok), F32),
            jax.ShapeDtypeStruct((dim, tok), BF16),
        ],
        scratch_shapes=[
            pltpu.VMEM((rows, dim), BF16), pltpu.VMEM(hsum.shape, BF16), pltpu.VMEM(hsum.shape, BF16),
            dma((1,)), dma((16,)), dma((16,)),
        ],
        compiler_params=params(56, collective_id=3, has_side_effects=True),
        cost_estimate=cost(2 * n * tok * dim * rows, 4 * n * tok * rows),
        name='logits',
    )(wt, x, lab, hsum)


def stats_kernel(n, st_ref, mask_ref, a_hbm, upt_hbm, down_hbm, out_ref, loss_ref, y_hbm, got, every, upt_buf, down_buf, a_buf,
                 y_buf, send1, recv1, send2, recv2, load_sem, a_sem, y_sem):
    me = lax.axis_index('stage')
    layers = upt_buf.shape[0]
    loads = [
        pltpu.make_async_copy(src, dst, load_sem.at[k])
        for k, (src, dst) in enumerate([(upt_hbm, upt_buf), (down_hbm, down_buf)])
    ]
    for load in loads:
        load.start()

    def load_a(m):
        start = pl.multiple_of((m + MLP_GATHER) * MLP_TILE, MLP_TILE)
        slot = lax.rem(m, 2)
        return pltpu.make_async_copy(a_hbm.at[:, pl.ds(start, MLP_TILE)], a_buf.at[slot], a_sem.at[slot])

    def store_y(m):
        slot = lax.rem(m, 2)
        start = pl.multiple_of(m * MLP_TILE, MLP_TILE)
        return pltpu.make_async_copy(y_buf.at[slot], y_hbm.at[:, pl.ds(start, MLP_TILE)], y_sem.at[slot])

    load_a(0).start()
    barrier = pltpu.get_barrier_semaphore()
    peers = [lax.rem(me + d, n) for d in range(n)]
    for d in range(1, n):
        pl.semaphore_signal(barrier, inc=1, device_id={'stage': peers[d]}, device_id_type=MESH)
    pl.semaphore_wait(barrier, n - 1)

    first = []
    for d in range(1, n):
        first.append(pltpu.make_async_remote_copy(
            src_ref=st_ref.at[peers[d]], dst_ref=got.at[d], send_sem=send1.at[d], recv_sem=recv1.at[d],
            device_id={'stage': peers[d]}, device_id_type=MESH))
        first[-1].start()

    weight = mask_ref[...]
    count = jnp.maximum(jnp.sum(weight, keepdims=True)[0], 1.0)
    second = [
        pltpu.make_async_remote_copy(
            src_ref=every.at[me], dst_ref=every.at[me], send_sem=send2.at[d], recv_sem=recv2.at[d],
            device_id={'stage': peers[d]}, device_id_type=MESH)
        for d in range(1, n)
    ]

    def reduce_stats():
        for copy in first:
            copy.wait()
        parts = [st_ref[me]] + [got[d] for d in range(1, n)]
        m = functools.reduce(jnp.maximum, [p[0:1] for p in parts])
        total = sum(p[1:2] * jnp.exp(p[0:1] - m) for p in parts)
        target = sum(p[2:3] for p in parts)
        w = mask_ref[me]
        scale = w / count
        term = w * (jnp.log(total) + m - target)
        every[me] = jnp.concatenate([m, scale / total, scale, term, jnp.zeros((4, m.shape[1]), F32)], axis=0)

    for load in loads:
        load.wait()
    tiles = MLP_STATS

    def piece(q, carry):
        m, i = q // layers, lax.rem(q, layers)
        slot = lax.rem(m, 2)

        @pl.when(i == 0)
        def _():
            @pl.when(m < tiles - 1)
            def _():
                load_a(m + 1).start()

            load_a(m).wait()

            @pl.when(m >= 2)
            def _():
                store_y(m - 2).wait()

            y_buf[slot] = a_buf[slot]

        @pl.when(is_middle())
        def _():
            y_buf[slot] = mlp_layer(y_buf[slot], upt_buf.at[i], down_buf.at[i])

        @pl.when(i == layers - 1)
        def _():
            store_y(m).start()

        @pl.when(q == 1)
        def _():
            reduce_stats()
            for copy in second:
                copy.start()

        return carry

    lax.fori_loop(0, tiles * layers, piece, 0)
    for copy in second:
        copy.wait()
    out_ref[...] = every[...]
    loss_ref[...] = jnp.broadcast_to(jnp.sum(every[:, 3, :], keepdims=True) / count, loss_ref.shape)
    for m in range(tiles - 2, tiles):
        store_y(m).wait()


def stats(st, mask, at, upt, down):
    n, _, tok = st.shape
    dim = at.shape[0]
    vmem = pl.BlockSpec(memory_space=pltpu.VMEM)
    anywhere = pl.BlockSpec(memory_space=pl.ANY)
    dma = pltpu.SemaphoreType.DMA
    return pl.pallas_call(
        functools.partial(stats_kernel, n),
        in_specs=[vmem, vmem] + [anywhere] * 3,
        out_specs=[vmem, vmem, anywhere],
        out_shape=[
            jax.ShapeDtypeStruct((n, 8, tok), F32),
            jax.ShapeDtypeStruct((8, 128), F32),
            jax.ShapeDtypeStruct((dim, MLP_STATS * MLP_TILE), BF16),
        ],
        scratch_shapes=[
            pltpu.VMEM((n, 8, tok), F32),
            pltpu.VMEM((n, 8, tok), F32),
            pltpu.VMEM(upt.shape, BF16),
            pltpu.VMEM(down.shape, BF16),
            pltpu.VMEM((2, dim, MLP_TILE), BF16),
            pltpu.VMEM((2, dim, MLP_TILE), BF16),
            dma((n,)), dma((n,)), dma((n,)), dma((n,)), dma((2,)), dma((2,)), dma((2,)),
        ],
        compiler_params=params(56, collective_id=0, has_side_effects=True),
        cost_estimate=cost(3e10, 2e7),
        name='stats',
    )(st, mask, at, upt, down)


def grad_kernel(n, e_hbm, w_hbm, x_hbm, a_hbm, upt_hbm, down_hbm, cm_ref, gs_ref, lab_ref, dx_ref, dw_hbm, y_hbm, g_buf, send_buf,
                own, pair, chain, load_sem, e_sem, pair_send, pair_recv, chain_send, chain_recv, a_sem, y_sem):
    stage = lax.axis_index('stage')
    chips = n // 2
    far = chips // 2
    z, core = stage // 2, lax.rem(stage, 2)
    dim, tok = dx_ref.shape
    rows = w_hbm.shape[1]
    half = dim // 2
    partner = {'stage': 2 * z + 1 - core}
    ahead = {'stage': 2 * lax.rem(z + 1, chips) + core}
    behind = {'stage': 2 * lax.rem(z + chips - 1, chips) + core}

    def chip_at(i):
        size = far - (i + 1) // 2
        sign = 2 * lax.rem(i, 2) - 1
        return lax.rem(z + sign * size + chips, chips)

    def block_at(i, own_side):
        return 2 * chip_at(i) + (core if own_side else 1 - core)

    def pair_copy(i):
        return pltpu.make_async_remote_copy(
            src_ref=send_buf.at[lax.rem(i, 2)], dst_ref=pair.at[i], send_sem=pair_send.at[lax.rem(i, 2)],
            recv_sem=pair_recv.at[i], device_id=partner, device_id_type=MESH)

    def pair_add(i):
        pair_copy(i).wait_recv()
        own[i] += pair[i]

    def unit(way, k, h, src):
        sl = pl.ds(h * half, half)
        s = way * 8 + k * 2 + h
        return pltpu.make_async_remote_copy(
            src_ref=src.at[sl, :], dst_ref=chain.at[way * far + k, sl, :], send_sem=chain_send.at[s], recv_sem=chain_recv.at[s],
            device_id=ahead if way == 0 else behind, device_id_type=MESH)

    def place(way, k):
        return 0 if k == 0 else 2 * k - 1 + way

    def first_send(way):
        unit(way, 0, way, own.at[0]).start()

    def plain_send(way):
        unit(way, 1, 1 - way, own.at[place(way, 1)]).start()

    def forward(way, k, h):
        here = chain.at[way * far + k]
        unit(way, k, h, here).wait_recv()
        sl = pl.ds(h * half, half)
        here[sl, :] += own[place(way, k + 1), sl, :]
        unit(way, k + 1, h, here).start()

    def gradients(w_buf, e_buf):
        def load_e(i, q):
            slot = lax.rem(i, 2)
            return pltpu.make_async_copy(e_hbm.at[block_at(i, q == 1)], e_buf.at[slot, q], e_sem.at[slot, q])

        for q in range(2):
            load_e(0, q).start()
        load_w = pltpu.make_async_copy(w_hbm, w_buf, load_sem.at[0])
        load_w.start()
        barrier = pltpu.get_barrier_semaphore()
        for peer in (partner, ahead, behind):
            pl.semaphore_signal(barrier, inc=1, device_id=peer, device_id_type=MESH)
        pl.semaphore_wait(barrier, 3)
        index = lax.broadcasted_iota(jnp.int32, (CHUNK, tok), 0)
        load_w.wait()

        def body(i, carry):
            @pl.when(i < chips - 1)
            def _():
                for q in range(2):
                    load_e(i + 1, q).start()

            @pl.when(i >= 2)
            def _():
                pair_copy(i - 2).wait_send()

            for q in range(2):
                load_e(i, q).wait()
            slot = lax.rem(i, 2)
            blocks = [block_at(i, q == 1) for q in range(2)]
            parts = [[], []]
            for q in range(2):
                gs, cm, lab = gs_ref[blocks[q]], cm_ref[blocks[q]], lab_ref[blocks[q]]
                m, over, scale = gs[0:1], gs[1:2], gs[2:3]
                for c in range(rows // CHUNK):
                    sl = pl.ds(c * CHUNK, CHUNK)
                    p = e_buf[slot, q, sl, :] * (jnp.exp(cm[c:c + 1] - m) * over)
                    g = jnp.where(index == lab - c * CHUNK, p - scale, p).astype(BF16)
                    g_buf[blocks[q], sl, :] = g
                    parts[q].append(g)
            both = jnp.concatenate([jnp.concatenate(p, axis=0) for p in parts], axis=1)
            dx = mm(w_buf[...], both, 1, 0)
            send_buf[slot] = dx[:, :tok]
            own[i] = dx[:, tok:]
            pair_copy(i).start()

            @pl.when(i >= 1)
            def _():
                pair_add(i - 1)

            @pl.when(i == 1)
            def _():
                first_send(0)
                first_send(1)

            @pl.when(i == 2)
            def _():
                plain_send(0)

            @pl.when(i == 3)
            def _():
                plain_send(1)

            @pl.when(i == chips - 2)
            def _():
                for way in range(2):
                    forward(way, 0, way)
            return carry

        lax.fori_loop(0, chips, body, 0)

    pl.run_scoped(gradients, pltpu.VMEM((dim, rows), BF16), pltpu.VMEM((2, 2, rows, tok), F32))
    pair_add(chips - 1)

    def fill(x_buf, upt_buf, down_buf, a_buf, y_buf, dw_buf):
        loads = [
            pltpu.make_async_copy(src, dst, load_sem.at[k])
            for k, (src, dst) in enumerate([(x_hbm, x_buf), (upt_hbm, upt_buf), (down_hbm, down_buf)])
        ]
        for load in loads:
            load.start()
        done = MLP_GATHER + MLP_STATS
        tiles = y_hbm.shape[1] // MLP_TILE

        def cols(m):
            return pl.ds(pl.multiple_of(m * MLP_TILE, MLP_TILE), MLP_TILE)

        def load_a(m):
            slot = lax.rem(m, 2)
            return pltpu.make_async_copy(a_hbm.at[:, cols(m + done)], a_buf.at[slot], a_sem.at[slot])

        def store_y(m):
            slot = lax.rem(m, 2)
            return pltpu.make_async_copy(y_buf.at[slot], y_hbm.at[:, cols(m)], y_sem.at[slot])

        load_a(0).start()
        loads[0].wait()
        width = 512
        pieces = rows // width

        def store_dw(j):
            slot = lax.rem(j, 2)
            start = pl.multiple_of(j * width, width)
            return pltpu.make_async_copy(dw_buf.at[slot], dw_hbm.at[:, pl.ds(start, width)], y_sem.at[slot])

        def head(j, carry):
            start = pl.multiple_of(j * width, width)
            g = jnp.concatenate([g_buf[b, pl.ds(start, width), :] for b in range(n)], axis=1)

            @pl.when(j >= 2)
            def _():
                store_dw(j - 2).wait()

            dw_buf[lax.rem(j, 2)] = mm(side_by_side(x_buf), g, 1, 1).astype(BF16)
            store_dw(j).start()

            @pl.when(j == 0)
            def _():
                for way in range(2):
                    forward(way, 1, 1 - way)

            @pl.when(j == 2)
            def _():
                for way in range(2):
                    forward(way, 1, way)

            @pl.when(j == 4)
            def _():
                for way in range(2):
                    forward(way, 2, 1 - way)

            @pl.when(j == pieces - 1)
            def _():
                for way in range(2):
                    forward(way, 2, way)
            return carry

        lax.fori_loop(0, pieces, head, 0)
        for j in range(pieces - 2, pieces):
            store_dw(j).wait()
        loads[1].wait()
        loads[2].wait()

        def layers(m, carry):
            slot = lax.rem(m, 2)

            @pl.when(m < tiles - 1)
            def _():
                load_a(m + 1).start()

            load_a(m).wait()

            @pl.when(m >= 2)
            def _():
                store_y(m - 2).wait()

            @pl.when(is_middle())
            def _():
                h = a_buf[slot]
                for i in range(upt_buf.shape[0]):
                    h = mlp_layer(h, upt_buf.at[i], down_buf.at[i])
                y_buf[slot] = h

            @pl.when(jnp.logical_not(is_middle()))
            def _():
                y_buf[slot] = a_buf[slot]

            store_y(m).start()
            return carry

        lax.fori_loop(0, tiles, layers, 0)
        for m in range(tiles - 2, tiles):
            store_y(m).wait()

    pl.run_scoped(
        fill, pltpu.VMEM(x_hbm.shape, BF16), pltpu.VMEM(upt_hbm.shape, BF16), pltpu.VMEM(down_hbm.shape, BF16),
        pltpu.VMEM((2, dim, MLP_TILE), BF16), pltpu.VMEM((2, dim, MLP_TILE), BF16), pltpu.VMEM((2, dim, 512), BF16))
    for h in range(2):
        for way in range(2):
            unit(way, far - 1, h, own.at[0]).wait_recv()
    dx_ref[...] = own[chips - 1] + (chain[far - 1] + chain[2 * far - 1])
    for i in range(chips - 2, chips):
        pair_copy(i).wait_send()
    for way in range(2):
        for k in range(far):
            for h in range(2):
                if k > 0 or h == way:
                    unit(way, k, h, own.at[0]).wait_send()


def grad(wt, e, x, at, upt, down, cm, gs, lab):
    dim, rows = wt.shape
    n, _, tok = e.shape
    chips = n // 2
    vmem = pl.BlockSpec(memory_space=pltpu.VMEM)
    anywhere = pl.BlockSpec(memory_space=pl.ANY)
    dma = pltpu.SemaphoreType.DMA
    return pl.pallas_call(
        functools.partial(grad_kernel, n),
        in_specs=[anywhere] * 6 + [vmem] * 3,
        out_specs=[vmem, anywhere, anywhere],
        out_shape=[
            jax.ShapeDtypeStruct((dim, tok), F32),
            jax.ShapeDtypeStruct((dim, rows), BF16),
            jax.ShapeDtypeStruct((dim, at.shape[1] - (MLP_GATHER + MLP_STATS) * MLP_TILE), BF16),
        ],
        scratch_shapes=[
            pltpu.VMEM((n, rows, tok), BF16),
            pltpu.VMEM((2, dim, tok), F32),
            pltpu.VMEM((chips, dim, tok), F32),
            pltpu.VMEM((chips, dim, tok), F32),
            pltpu.VMEM((chips, dim, tok), F32),
            dma((3,)), dma((2, 2)), dma((2,)), dma((chips,)), dma((16,)), dma((16,)), dma((2,)), dma((2,)),
        ],
        compiler_params=pltpu.CompilerParams(vmem_limit_bytes=63 * MIB, collective_id=1, has_side_effects=True),
        cost_estimate=cost(6 * n * tok * dim * rows, 6 * n * tok * rows),
        name='grad',
    )(e, wt, x, at, upt, down, cm, gs, lab)


def solution(mesh):
    n = mesh.shape['stage']
    row_spec = P(('data', 'stage'), None)
    vocab_spec = P('stage', None)
    layer_spec = P('stage', None, None, None)
    acts_spec = P(('data', 'stage'), None, None)

    def per_device(x_loc, w_loc, labels, loss_mask, e_loc, next_ids, acts_loc, up_loc, down_loc):
        tok = x_loc.shape[0]
        offset = lax.axis_index('stage') * w_loc.shape[0]
        wt, at, down = w_loc.T, acts_loc[0].T, jnp.swapaxes(down_loc[0], 1, 2)
        ids = (next_ids - offset).reshape(n, 1, tok)
        lab = (labels - offset).reshape(n, 1, tok)
        mask = loss_mask.astype(F32).reshape(n, 1, tok)
        x, hsum, y0, upt = gather(x_loc.T, ids, e_loc.T, up_loc[0], down, at)
        e, cm, st, embed_rows = logits(wt, x, lab, hsum)
        gs, loss, y1 = stats(st, mask, at, upt, down)
        dx, dw, y2 = grad(wt, e, x, at, upt, down, cm, gs, lab)
        stage_out = jnp.concatenate([y0, y1, y2], axis=1)
        return loss[0, :1], dx.T, dw.T, embed_rows.T, stage_out.T[None]

    return jax.shard_map(
        per_device,
        mesh=mesh,
        in_specs=(row_spec, vocab_spec, P('data'), P('data'), vocab_spec, P('data'), acts_spec, layer_spec, layer_spec),
        out_specs=(P('data'), row_spec, row_spec, row_spec, acts_spec),
        check_vma=False,
    )
```
